256 devices in a mesh: mem: 8 (over z_lo, y), col: 32 (over z_hi, x, core).
Axes of the slice: x: 4, y: 4, z: 8 (z_hi: 4, z_lo: 2; z = z_hi * 2 + z_lo), core: 2. Of those that a mesh axis runs over, the one named last changes fastest.
Arguments:
- perturbations: bfloat16 [4, 256, 512, 256], P(None, 'mem', 'col'), may hold values from -4 to 4
- loc_weights: float32 [7], replicated, may hold values from 0.3 to 1
- offsets: int32 [7, 2], replicated, may hold values from -4 to 4, as said below
- obs_x: int32 [65536], P('col'), may hold values from 0 to 511, as said below
- obs_y: int32 [65536], P('col'), may hold values from 0 to 255
- obs_t: int32 [65536], P('col'), may hold values from 0 to 3
- innovations: float32 [65536], P('col'), may hold values from -6 to 6
- obs_rinv: float32 [65536], P('col'), may hold values from 0.5 to 6
Outputs:
- control: float32 [256, 512, 256], P('mem', 'col')
- increment: float32 [4, 512, 256], P(None, 'col')
The draws below stay inside these ranges and needn't reach their ends.
Inputs may be any that keep to these rules, and one draw needn't show every extreme that they name: `obs_x`: observation o lies in the columns (o // 2048) * 16 to (o // 2048) * 16 + 15. `offsets`: column 0 gives the offset along the first grid dimension, column 1 along the second; along the first both -4 and 4 occur.
All inputs are finite; a program needn't handle non-finite values.
Results may differ from the reference program's by a relative error of at most 0.00035.
Values may be sent and summed in bfloat16 or wider, within the bound.
A program may use at most 64 MiB of HBM per device.

```python
import math
import jax
import jax.numpy as jnp
from jax import lax

K = 256
L = 4
CX = 16
NY = 256
NOBS_DEV = 2048
TAPS = 7
RADIUS = 4
ITERS = 3
NX = 512
NOBS = 65536


def draw_perturbations(key, part):
    subkeys = jax.random.split(jax.random.fold_in(key, 11), 1)
    member_scale = (0.5 + jnp.arange(K, dtype=jnp.float32) / K).reshape(1, K, 1, 1)
    values = jax.random.truncated_normal(subkeys[0], -4.0, 4.0, (L, K, NX, NY), jnp.float32)
    return (values * member_scale / jnp.sqrt(K * 1.0)).astype(jnp.bfloat16)


def draw_offsets(key, part):
    subkeys = jax.random.split(jax.random.fold_in(key, 23), 2)
    along = jax.random.randint(subkeys[0], (TAPS,), -RADIUS, RADIUS + 1, jnp.int32)
    along = along.at[0].set(0).at[1].set(RADIUS).at[2].set(-RADIUS)
    across = jax.random.randint(subkeys[1], (TAPS,), -RADIUS, RADIUS + 1, jnp.int32)
    across = across.at[0].set(0)
    return jnp.stack([along, across], axis=1).astype(jnp.int32)


def draw_obs_x(key, part):
    owners = jnp.arange(NOBS, dtype=jnp.int32) // NOBS_DEV
    within = jax.random.randint(jax.random.fold_in(key, 37), (NOBS,), 0, CX, jnp.int32)
    return (owners * CX + within).astype(jnp.int32)


def draw_obs_rinv(key, part):
    subkey = jax.random.fold_in(key, 41)
    rising = 1.0 + 2.0 * jnp.arange(NOBS, dtype=jnp.float32) / NOBS
    base = jnp.exp(jax.random.uniform(subkey, (NOBS,), jnp.float32, jnp.log(0.5), jnp.log(2.0)))
    return (base * rising).astype(jnp.float32)


def place_ends(array, rng, smallest, largest):
    shape = array.shape
    index_at = [jax.random.randint(jax.random.fold_in(rng, axis), (), 0, shape[axis]) for axis in range(len(shape))]
    array = array.at[tuple(index_at)].set(smallest)
    longest = shape.index(max(shape))
    index_at[longest] = (index_at[longest] + 1) % shape[longest]
    return array.at[tuple(index_at)].set(largest)


def shard_levels(rng, shape, pieces, low, largest):
    level, own = 1.0, jax.random.fold_in(rng, 6)
    for position, blocks in pieces:
        heights = jnp.exp(jax.random.uniform(jax.random.fold_in(own, position), (blocks,), jnp.float32, low / len(pieces), largest / len(pieces)))
        level = level * jnp.repeat(heights, shape[position] // blocks).reshape([-1 if axis == position else 1 for axis in range(len(shape))])
    return level


def gaussian(rng, shape, scale, bound, cuts=(), kind=jnp.bfloat16):
    result = scale * jax.random.normal(rng, shape, jnp.float32)
    if cuts:
        result = result * shard_levels(rng, shape, cuts, -0.22, 0.18)
    return jnp.clip(result, -bound, bound).astype(kind)


def setup_inputs(seed: int = 0) -> dict:
    key_of = jax.random.split(jax.random.key(seed), 9)
    return {
        "perturbations": draw_perturbations(jax.random.fold_in(key_of[8], 71), 0),
        "loc_weights": jnp.clip(jnp.exp(jax.random.uniform(key_of[1], (TAPS,), jnp.float32, math.log(0.3), math.log(1.0))), 0.3, 1.0),
        "offsets": draw_offsets(jax.random.fold_in(key_of[8], 71), 0),
        "obs_x": draw_obs_x(jax.random.fold_in(key_of[8], 71), 0),
        "obs_y": place_ends(jax.random.randint(key_of[4], (NOBS,), 0, NY), jax.random.fold_in(key_of[4], 1), 0, NY - 1).astype(jnp.int32),
        "obs_t": place_ends(jax.random.randint(key_of[5], (NOBS,), 0, L), jax.random.fold_in(key_of[5], 1), 0, L - 1).astype(jnp.int32),
        "innovations": gaussian(key_of[6], (NOBS,), 1.0, 6.0, ((0, 32),), jnp.float32),
        "obs_rinv": draw_obs_rinv(jax.random.fold_in(key_of[8], 71), 0),
    }


def pad_columns(source):
    return jnp.pad(source, ((0, 0), (RADIUS, RADIUS), (0, 0)))


def apply_taps(padded, loc_weights, offsets, mirror):
    length = padded.shape[1] - 2 * RADIUS
    summed = jnp.zeros((padded.shape[0], length, padded.shape[2]), jnp.float32)
    for tap_index in range(TAPS):
        along = offsets[tap_index, 0]
        across = offsets[tap_index, 1]
        if mirror:
            along = -along
            across = -across
        moved = lax.dynamic_slice_in_dim(padded, (RADIUS + along).astype(jnp.int32), length, 1)
        summed = summed + loc_weights[tap_index] * jnp.roll(moved, -across, axis=2)
    return summed


def combine(perturbations, coeffs):
    return jnp.stack([jnp.sum(perturbations[level].astype(jnp.float32) * coeffs, axis=0) for level in range(L)])


def reference(perturbations, loc_weights, offsets, obs_x, obs_y, obs_t, innovations, obs_rinv):
    flat_index = ((obs_t * NX + obs_x) * NY + obs_y).astype(jnp.int32)

    def forward(control):
        return combine(perturbations, apply_taps(pad_columns(control), loc_weights, offsets, False))

    def adjoint(values):
        weighted = jnp.zeros((L * NX * NY,), jnp.float32).at[flat_index].add(values).reshape(L, NX, NY)
        products = perturbations[0].astype(jnp.float32) * weighted[0][None]
        for level in range(1, L):
            products = products + perturbations[level].astype(jnp.float32) * weighted[level][None]
        return apply_taps(pad_columns(products), loc_weights, offsets, True)

    gradient = adjoint(obs_rinv * innovations)
    control = jnp.zeros_like(gradient)
    residual = gradient
    direction = gradient
    norm_now = jnp.sum(residual * residual)
    for turn_index in range(ITERS):
        observed = forward(direction).reshape(-1)[flat_index]
        image = direction + adjoint(obs_rinv * observed)
        step_size = norm_now / jnp.sum(direction * image)
        control = control + step_size * direction
        if turn_index + 1 < ITERS:
            residual = residual - step_size * image
            norm_next = jnp.sum(residual * residual)
            direction = residual + (norm_next / norm_now) * direction
            norm_now = norm_next
    increment = forward(control)
    return (control, increment)
```

```python
import jax
import jax.numpy as jnp
from jax import lax
from jax.experimental import pallas as pl
from jax.experimental.pallas import tpu as pltpu
from jax.sharding import PartitionSpec as P

TAPS = 7
RADIUS = 4
LANES = 128
HALO = 2 * RADIUS
F32 = jnp.float32
MESH = pl.DeviceIdType.MESH


def make_kernel(groups, blocks, levels, members, width, depth, obs_rows):
    halves = depth // LANES
    planes = levels * halves
    rows = width + 2 * HALO
    own = pl.ds(HALO, width)
    low_rows = pl.ds(0, HALO)
    high_rows = pl.ds(HALO + width, HALO)
    last_own = pl.ds(width, HALO)
    first_own = pl.ds(HALO, HALO)

    def kernel(
        pert, weights, offsets, obs_x, obs_y, obs_t, innov, rinv,
        control, increment,
        p, p_low, p_high, fields, z, mixed, resid, second, part, gathered, full,
        note, group_note, sums, block_note,
        load_sem, halo_send, halo_recv, field_send, field_recv,
        rs_send, rs_recv, ag_send, ag_recv, low_send, low_recv, high_send, high_recv,
        note_send, note_recv, sum_send, sum_recv,
    ):
        me = lax.axis_index("mem")
        col = lax.axis_index("col")
        right = lax.rem(col + 1, blocks)
        left = lax.rem(col + blocks - 1, blocks)

        barrier = pltpu.get_barrier_semaphore()

        def greet(target):
            pl.semaphore_signal(barrier, inc=1, device_id=target, device_id_type=MESH)

        load = pltpu.make_async_copy(pert, p, load_sem)
        load.start()
        for step in range(1, groups):
            greet((lax.rem(me + step, groups), col))
        for other in range(groups):
            greet((other, right))
            greet((other, left))

        def greet_block(step, carry):
            greet((me, lax.rem(col + step, blocks)))
            return carry

        lax.fori_loop(1, blocks, greet_block, 0)

        lanes8 = lax.broadcasted_iota(jnp.int32, (1, LANES), 1)
        cell_rows = lax.broadcasted_iota(jnp.int32, (levels * width, LANES), 0)
        depth_rows = lax.broadcasted_iota(jnp.int32, (depth, LANES), 0)

        def place(chunk, total):
            at = pl.ds(chunk, 1)
            cell = obs_t[at, :] * width + (obs_x[at, :] - col * width)
            r = rinv[at, :]
            hit = cell_rows == cell
            pieces = []
            for value in (r * innov[at, :], r):
                rest = value
                for _ in range(3):
                    piece = rest.astype(jnp.bfloat16)
                    rest = rest - piece.astype(F32)
                    pieces.append(jnp.where(hit, piece.astype(F32), 0.0).astype(jnp.bfloat16))
            left_side = jnp.concatenate(pieces, axis=0)
            right_side = jnp.where(depth_rows == obs_y[at, :], 1.0, 0.0).astype(jnp.bfloat16)
            return total + lax.dot_general(
                left_side, right_side, (((1,), (1,)), ((), ())), preferred_element_type=F32
            )

        spread = lax.fori_loop(
            0, obs_rows, place, jnp.zeros((6 * levels * width, depth), F32)
        )
        cells = levels * width
        for which in range(2):
            base = 3 * which * cells
            summed = (
                spread[base : base + cells]
                + spread[base + cells : base + 2 * cells]
                + spread[base + 2 * cells : base + 3 * cells]
            )
            for level in range(levels):
                for half in range(halves):
                    fields[which, level * halves + half, own, :] = summed[
                        level * width : (level + 1) * width, half * LANES : (half + 1) * LANES
                    ]

        pl.semaphore_wait(barrier, groups - 1 + 2 * groups + blocks - 1)

        def remote(source, target, send, recv, device):
            return pltpu.make_async_remote_copy(
                src_ref=source, dst_ref=target, send_sem=send, recv_sem=recv,
                device_id=device, device_id_type=MESH,
            )

        to_right = remote(
            pert.at[:, :, pl.ds(width - HALO, HALO), :], p_low, halo_send.at[0], halo_recv.at[0], (me, right)
        )
        to_left = remote(
            pert.at[:, :, pl.ds(0, HALO), :], p_high, halo_send.at[1], halo_recv.at[1], (me, left)
        )
        to_right.start()
        to_left.start()
        fields_right = remote(
            fields.at[:, :, last_own, :], fields.at[:, :, low_rows, :],
            field_send.at[0], field_recv.at[0], (me, right),
        )
        fields_left = remote(
            fields.at[:, :, first_own, :], fields.at[:, :, high_rows, :],
            field_send.at[1], field_recv.at[1], (me, left),
        )
        fields_right.start()
        fields_left.start()

        tap_weight = [weights[s] for s in range(TAPS)]
        along = [offsets[2 * s] for s in range(TAPS)]
        across = [offsets[2 * s + 1] for s in range(TAPS)]

        def shifted(pair, amount):
            turn = jnp.where(amount < 0, amount + LANES, amount)
            turned = [pltpu.roll(v, turn, 1) for v in pair]
            spot = lax.broadcasted_iota(jnp.int32, pair[0].shape, 1) - amount
            inside = (spot >= 0) & (spot < LANES)
            return [
                jnp.where(inside, turned[h], turned[1 - h]) for h in range(halves)
            ]

        def mix(source, at, k):
            for half in range(halves):
                total = None
                for level in range(levels):
                    term = source[level, k, :, half * LANES : (half + 1) * LANES].astype(F32) * z[
                        level * halves + half, at, :
                    ]
                    total = term if total is None else total + term
                mixed[k, half, at, :] = total

        def mix_own():
            def step(k, carry):
                for more in range(2):
                    mix(p, own, 2 * k + more)
                return carry

            lax.fori_loop(0, members // 2, step, 0)

        def mix_edges():
            def step(k, carry):
                for more in range(2):
                    mix(p_low, low_rows, 2 * k + more)
                    mix(p_high, high_rows, 2 * k + more)
                return carry

            lax.fori_loop(0, members // 2, step, 0)

        reach = width + 2 * RADIUS
        row_at = lax.broadcasted_iota(jnp.int32, (reach, LANES), 0) + (col * width - RADIUS)
        keep = jnp.where((row_at >= 0) & (row_at < blocks * width), 1.0, 0.0)

        def transpose_taps(turn):
            def step(k, carry):
                total = [jnp.zeros((reach, LANES), F32) for _ in range(halves)]
                for s in range(TAPS):
                    start = RADIUS - along[s]
                    pair = [mixed[k, half, pl.ds(start, reach), :] for half in range(halves)]
                    moved = shifted(pair, across[s])
                    total = [total[half] + tap_weight[s] * moved[half] for half in range(halves)]
                for half in range(halves):
                    resid[turn, k, half, pl.ds(RADIUS, reach), :] = total[half] * keep
                return carry

            lax.fori_loop(0, members, step, 0)

        def taps_and_sum(turn):
            def step(k, sums_so_far):
                total = [jnp.zeros((width, LANES), F32) for _ in range(halves)]
                for s in range(TAPS):
                    start = HALO + along[s]
                    pair = [resid[turn, k, half, pl.ds(start, width), :] for half in range(halves)]
                    moved = shifted(pair, -across[s])
                    total = [total[half] + tap_weight[s] * moved[half] for half in range(halves)]
                return tuple(
                    sums_so_far[level * halves + half]
                    + p[level, k, :, half * LANES : (half + 1) * LANES].astype(F32) * total[half]
                    for level in range(levels)
                    for half in range(halves)
                )

            summed = lax.fori_loop(
                0, members, step, tuple(jnp.zeros((width, LANES), F32) for _ in range(planes))
            )
            for plane in range(planes):
                part[turn, plane] = summed[plane]

        def chunk_copy(turn, step):
            peer = lax.rem(me + step, groups)
            return remote(
                part.at[turn, peer], gathered.at[turn, step - 1],
                rs_send.at[turn, step - 1], rs_recv.at[turn, step - 1], (peer, col),
            )

        def whole_copy(turn, step, sender, peer):
            spot = full.at[turn, sender, own, :]
            return remote(
                spot, spot, ag_send.at[turn, step - 1], ag_recv.at[turn, step - 1], (peer, col)
            )

        def edge_copies(turn, other, sender, slot):
            return (
                remote(
                    full.at[turn, sender, last_own, :], full.at[turn, sender, low_rows, :],
                    low_send.at[turn, other], low_recv.at[turn, slot], (other, right),
                ),
                remote(
                    full.at[turn, sender, first_own, :], full.at[turn, sender, high_rows, :],
                    high_send.at[turn, other], high_recv.at[turn, slot], (other, left),
                ),
            )

        def note_copy(which, step, sender, peer):
            return remote(
                note.at[which], group_note.at[which, sender],
                note_send.at[which, step - 1], note_recv.at[which, step - 1], (peer, col),
            )

        def sum_copy(which, step, sender, peer):
            return remote(
                sums.at[which], block_note.at[which, sender],
                sum_send.at[which, step - 1], sum_recv.at[which, step - 1], (me, peer),
            )

        def start_sums(turn):
            def step(s, carry):
                chunk_copy(turn, s).start()
                return carry

            lax.fori_loop(1, groups, step, 0)

        def finish_sums(turn):
            def step(s, carry):
                chunk_copy(turn, s).wait_recv()
                return carry

            lax.fori_loop(1, groups, step, 0)
            total = part[turn, me]
            for s in range(groups - 1):
                total = total + gathered[turn, s]
            full[turn, me, own, :] = total
            return total

        def start_spread(turn, edges):
            def step(s, carry):
                whole_copy(turn, s, me, lax.rem(me + s, groups)).start()
                return carry

            lax.fori_loop(1, groups, step, 0)
            if edges:

                def edge_step(other, carry):
                    for copy in edge_copies(turn, other, me, me):
                        copy.start()
                    return carry

                lax.fori_loop(0, groups, edge_step, 0)

        def finish_own(turn):
            def step(s, carry):
                peer = lax.rem(me + groups - s, groups)
                whole_copy(turn, s, peer, peer).wait_recv()
                return carry

            lax.fori_loop(1, groups, step, 0)

        def finish_edges(turn):
            def step(other, carry):
                for copy in edge_copies(turn, other, other, other):
                    copy.wait_recv()
                return carry

            lax.fori_loop(0, groups, step, 0)

        def send_note(which, values):
            row = jnp.zeros((1, LANES), F32)
            for at, value in enumerate(values):
                row = jnp.where(lanes8 == at, value, row)
            note[which] = row
            group_note[which, me] = row

            def step(s, carry):
                note_copy(which, s, me, lax.rem(me + s, groups)).start()
                return carry

            lax.fori_loop(1, groups, step, 0)

        def pass_note(which):
            def step(s, carry):
                peer = lax.rem(me + groups - s, groups)
                note_copy(which, s, peer, peer).wait_recv()
                return carry

            lax.fori_loop(1, groups, step, 0)
            total = group_note[which, 0]
            for other in range(1, groups):
                total = total + group_note[which, other]
            sums[which] = total
            block_note[which, col] = total

            def send(s, carry):
                sum_copy(which, s, col, lax.rem(col + s, blocks)).start()
                return carry

            lax.fori_loop(1, blocks, send, 0)

        def read_note(which, count):
            def step(s, carry):
                peer = lax.rem(col + blocks - s, blocks)
                sum_copy(which, s, peer, peer).wait_recv()
                return carry

            lax.fori_loop(1, blocks, step, 0)
            total = block_note[which, 0]
            for other in range(1, blocks):
                total = total + block_note[which, other]
            return [
                jnp.sum(jnp.where(lanes8 == at, total, 0.0), axis=1, keepdims=True)
                for at in range(count)
            ]

        def all_of(value):
            return jnp.sum(jnp.sum(value, axis=0, keepdims=True), axis=1, keepdims=True)

        load.wait()
        for plane in range(planes):
            z[plane, own, :] = fields[0, plane, own, :]
        mix_own()
        fields_right.wait_recv()
        fields_left.wait_recv()
        has_left = jnp.where(col > 0, 1.0, 0.0)
        has_right = jnp.where(col < blocks - 1, 1.0, 0.0)
        for which in range(2):
            for plane in range(planes):
                fields[which, plane, low_rows, :] = fields[which, plane, low_rows, :] * has_left
                fields[which, plane, high_rows, :] = fields[which, plane, high_rows, :] * has_right
        for plane in range(planes):
            z[plane, low_rows, :] = fields[0, plane, low_rows, :]
            z[plane, high_rows, :] = fields[0, plane, high_rows, :]
        to_right.wait_recv()
        to_left.wait_recv()
        mix_edges()
        transpose_taps(0)
        taps_and_sum(0)
        start_sums(0)

        def square(k, total):
            for half in range(halves):
                value = resid[0, k, half, own, :]
                total = total + value * value
            return total

        norm = all_of(lax.fori_loop(0, members, square, jnp.zeros((width, LANES), F32)))
        mine = finish_sums(0)
        start_spread(0, True)
        send_note(0, [norm, all_of(fields[1, me, own, :] * mine * mine)])
        finish_own(0)
        pass_note(0)

        def image_of_first(at):
            for plane in range(planes):
                z[plane, at, :] = (
                    fields[0, plane, at, :] + fields[1, plane, at, :] * full[0, plane, at, :]
                )

        image_of_first(own)
        mix_own()
        finish_edges(0)
        image_of_first(low_rows)
        image_of_first(high_rows)
        mix_edges()
        transpose_taps(1)
        taps_and_sum(1)
        start_sums(1)
        finish_sums(1)
        start_spread(1, True)
        norm_0, bend_0 = read_note(0, 2)
        curve_0 = norm_0 + bend_0
        step_0 = norm_0 / curve_0
        finish_own(1)

        def image_of_second(at):
            for plane in range(planes):
                z[plane, at, :] = (fields[0, plane, at, :] - step_0 * z[plane, at, :]) + fields[
                    1, plane, at, :
                ] * (full[0, plane, at, :] - step_0 * full[1, plane, at, :])

        image_of_second(own)
        mix_own()
        finish_edges(1)
        image_of_second(low_rows)
        image_of_second(high_rows)
        mix_edges()
        transpose_taps(2)
        taps_and_sum(2)
        start_sums(2)

        def products(k, so_far):
            ab, ac, bb, bc, cc = so_far
            for half in range(halves):
                a = resid[0, k, half, own, :]
                b = a - step_0 * resid[1, k, half, own, :]
                c = resid[2, k, half, own, :]
                second[k, half] = b
                ab, ac, bb, bc, cc = ab + a * b, ac + a * c, bb + b * b, bc + b * c, cc + c * c
            return ab, ac, bb, bc, cc

        inner = [
            all_of(v)
            for v in lax.fori_loop(
                0, members, products, tuple(jnp.zeros((width, LANES), F32) for _ in range(5))
            )
        ]
        mine_c = finish_sums(2)
        start_spread(2, False)
        mine_a = full[0, me, own, :]
        mine_b = mine_a - step_0 * full[1, me, own, :]
        weight = fields[1, me, own, :]
        wb, wc = weight * mine_b, weight * mine_c
        bends = [all_of(v) for v in (wb * mine_a, wc * mine_a, wb * mine_b, wc * mine_b, wc * mine_c)]
        send_note(1, inner + bends)
        pass_note(1)
        g_ab, g_ac, g_bb, g_bc, g_cc, e_ab, e_ac, e_bb, e_bc, e_cc = read_note(1, 10)
        finish_own(2)

        def form(aa, ab, ac, bb, bc, cc, u):
            a, b, c = u
            return (
                a * a * aa + b * b * bb + c * c * cc + 2.0 * (a * b * ab + a * c * ac + b * c * bc)
            )

        h = (curve_0, g_ab + e_ab, g_ac + e_ac, g_bb + e_bb, g_bc + e_bc, g_cc + e_cc)
        one = jnp.ones_like(norm_0)
        ratio_0 = g_bb / norm_0
        d1 = (ratio_0, one, 0.0 * one)
        step_1 = g_bb / form(*h, d1)
        mixing = step_1 * ratio_0 / step_0
        r2 = (-mixing, one + mixing, -step_1)
        norm_2 = form(norm_0, g_ab, g_ac, g_bb, g_bc, g_cc, r2)
        ratio_1 = norm_2 / g_bb
        d2 = tuple(r + ratio_1 * d for r, d in zip(r2, d1))
        step_2 = norm_2 / form(*h, d2)
        in_a = step_0 + step_1 * d1[0] + step_2 * d2[0]
        in_b = step_1 * d1[1] + step_2 * d2[1]
        in_c = step_1 * d1[2] + step_2 * d2[2]

        def write(k, carry):
            for half in range(halves):
                control[k, :, half * LANES : (half + 1) * LANES] = (
                    in_a * resid[0, k, half, own, :]
                    + in_b * second[k, half]
                    + in_c * resid[2, k, half, own, :]
                )
            return carry

        lax.fori_loop(0, members, write, 0)
        for level in range(levels):
            for half in range(halves):
                plane = level * halves + half
                a = full[0, plane, own, :]
                b = a - step_0 * full[1, plane, own, :]
                increment[level, :, half * LANES : (half + 1) * LANES] = (
                    in_a * a + in_b * b + in_c * full[2, plane, own, :]
                )

        for copy in (to_right, to_left, fields_right, fields_left):
            copy.wait_send()
        for turn in range(3):

            def settle(s, carry):
                chunk_copy(turn, s).wait_send()
                whole_copy(turn, s, me, lax.rem(me + s, groups)).wait_send()
                return carry

            lax.fori_loop(1, groups, settle, 0)
        for turn in range(2):

            def settle_edges(other, carry):
                for copy in edge_copies(turn, other, me, me):
                    copy.wait_send()
                return carry

            lax.fori_loop(0, groups, settle_edges, 0)

            def settle_notes(s, carry):
                note_copy(turn, s, me, lax.rem(me + s, groups)).wait_send()
                return carry

            lax.fori_loop(1, groups, settle_notes, 0)

            def settle_blocks(s, carry):
                sum_copy(turn, s, col, lax.rem(col + s, blocks)).wait_send()
                return carry

            lax.fori_loop(1, blocks, settle_blocks, 0)

    bf16 = jnp.bfloat16
    dma = pltpu.SemaphoreType.DMA
    scratch = [
        pltpu.VMEM((levels, members, width, depth), bf16),
        pltpu.VMEM((levels, members, HALO, depth), bf16),
        pltpu.VMEM((levels, members, HALO, depth), bf16),
        pltpu.VMEM((2, planes, rows, LANES), F32),
        pltpu.VMEM((planes, rows, LANES), F32),
        pltpu.VMEM((members, halves, rows, LANES), F32),
        pltpu.VMEM((3, members, halves, rows, LANES), F32),
        pltpu.VMEM((members, halves, width, LANES), F32),
        pltpu.VMEM((3, planes, width, LANES), F32),
        pltpu.VMEM((3, groups - 1, width, LANES), F32),
        pltpu.VMEM((3, planes, rows, LANES), F32),
        pltpu.VMEM((2, 1, LANES), F32),
        pltpu.VMEM((2, groups, 1, LANES), F32),
        pltpu.VMEM((2, 1, LANES), F32),
        pltpu.VMEM((2, blocks, 1, LANES), F32),
        dma,
        dma((2,)), dma((2,)), dma((2,)), dma((2,)),
        dma((3, groups - 1)), dma((3, groups - 1)), dma((3, groups - 1)), dma((3, groups - 1)),
        dma((2, groups)), dma((2, groups)), dma((2, groups)), dma((2, groups)),
        dma((2, groups - 1)), dma((2, groups - 1)), dma((2, blocks - 1)), dma((2, blocks - 1)),
    ]
    return kernel, scratch


def solution(mesh):
    groups, blocks = mesh.shape["mem"], mesh.shape["col"]

    def per_device(perturbations, loc_weights, offsets, obs_x, obs_y, obs_t, innovations, obs_rinv):
        levels, members, width, depth = perturbations.shape
        obs_rows = obs_x.shape[0] // LANES
        kernel, scratch = make_kernel(groups, blocks, levels, members, width, depth, obs_rows)
        vmem = pl.BlockSpec(memory_space=pltpu.VMEM)
        smem = pl.BlockSpec(memory_space=pltpu.SMEM)
        return pl.pallas_call(
            kernel,
            out_shape=(
                jax.ShapeDtypeStruct((members, width, depth), F32),
                jax.ShapeDtypeStruct((levels, width, depth), F32),
            ),
            in_specs=[pl.BlockSpec(memory_space=pl.ANY), smem, smem] + [vmem] * 5,
            out_specs=(vmem, vmem),
            scratch_shapes=scratch,
            compiler_params=pltpu.CompilerParams(collective_id=0, has_side_effects=True),
        )(
            perturbations, loc_weights, offsets.reshape(-1),
            *(v.reshape(obs_rows, LANES) for v in (obs_x, obs_y, obs_t, innovations, obs_rinv)),
        )

    return jax.shard_map(
        per_device,
        mesh=mesh,
        in_specs=(P(None, "mem", "col", None), P(), P()) + (P("col"),) * 5,
        out_specs=(P("mem", "col", None), P(None, "col", None)),
        check_vma=False,
    )
```

```python
import jax
import jax.numpy as jnp
from jax import lax
from jax.experimental import pallas as pl
from jax.experimental.pallas import tpu as pltpu
from jax.sharding import PartitionSpec as P

TAPS = 7
RADIUS = 4
LANES = 128
HALO = 2 * RADIUS
F32 = jnp.float32
UNROLL = 4
TAP_UNROLL = 4
MESH = pl.DeviceIdType.MESH


def make_kernel(groups, blocks, levels, members, width, depth, obs_rows):
    halves = depth // LANES
    planes = levels * halves
    rows = width + 2 * HALO
    own = pl.ds(HALO, width)
    low_rows = pl.ds(0, HALO)
    high_rows = pl.ds(HALO + width, HALO)
    last_own = pl.ds(width, HALO)
    first_own = pl.ds(HALO, HALO)

    def kernel(
        pert, weights, offsets, obs_x, obs_y, obs_t, innov, rinv,
        out_a, out_b, out_c, inc_a, inc_b, inc_c, coefficients,
        p, p_low, p_high, fields, z, mixed, resid, second, part, gathered, full,
        note, group_note, sums, block_note,
        load_sem, out_sem, mixed_send, mixed_recv, halo_send, halo_recv, field_send, field_recv,
        rs_send, rs_recv, ag_send, ag_recv, low_send, low_recv, high_send, high_recv,
        note_send, note_recv, sum_send, sum_recv,
    ):
        me = lax.axis_index("mem")
        col = lax.axis_index("col")
        right = lax.rem(col + 1, blocks)
        left = lax.rem(col + blocks - 1, blocks)

        barrier = pltpu.get_barrier_semaphore()

        def greet(target):
            pl.semaphore_signal(barrier, inc=1, device_id=target, device_id_type=MESH)

        load = pltpu.make_async_copy(pert, p, load_sem)
        load.start()
        for step in range(1, groups):
            greet((lax.rem(me + step, groups), col))
        for other in range(groups):
            greet((other, right))
            greet((other, left))

        def greet_block(step, carry):
            greet((me, lax.rem(col + step, blocks)))
            return carry

        lax.fori_loop(1, blocks, greet_block, 0)

        lanes8 = lax.broadcasted_iota(jnp.int32, (1, LANES), 1)
        cell_rows = lax.broadcasted_iota(jnp.int32, (levels * width, LANES), 0)
        depth_rows = lax.broadcasted_iota(jnp.int32, (depth, LANES), 0)

        def place(chunk, total):
            at = pl.ds(chunk, 1)
            cell = obs_t[at, :] * width + (obs_x[at, :] - col * width)
            r = rinv[at, :]
            hit = cell_rows == cell
            pieces = []
            for value in (r * innov[at, :], r):
                rest = value
                for _ in range(3):
                    piece = rest.astype(jnp.bfloat16)
                    rest = rest - piece.astype(F32)
                    pieces.append(jnp.where(hit, piece.astype(F32), 0.0).astype(jnp.bfloat16))
            left_side = jnp.concatenate(pieces, axis=0)
            right_side = jnp.where(depth_rows == obs_y[at, :], 1.0, 0.0).astype(jnp.bfloat16)
            return total + lax.dot_general(
                left_side, right_side, (((1,), (1,)), ((), ())), preferred_element_type=F32
            )

        spread = lax.fori_loop(
            0, obs_rows, place, jnp.zeros((6 * levels * width, depth), F32)
        )
        cells = levels * width
        for which in range(2):
            base = 3 * which * cells
            summed = (
                spread[base : base + cells]
                + spread[base + cells : base + 2 * cells]
                + spread[base + 2 * cells : base + 3 * cells]
            )
            for level in range(levels):
                for half in range(halves):
                    fields[which, level * halves + half, own, :] = summed[
                        level * width : (level + 1) * width, half * LANES : (half + 1) * LANES
                    ]

        def remote(source, target, send, recv, device):
            return pltpu.make_async_remote_copy(
                src_ref=source, dst_ref=target, send_sem=send, recv_sem=recv,
                device_id=device, device_id_type=MESH,
            )

        to_right = remote(
            pert.at[:, :, pl.ds(width - HALO, HALO), :], p_low, halo_send.at[0], halo_recv.at[0], (me, right)
        )
        to_left = remote(
            pert.at[:, :, pl.ds(0, HALO), :], p_high, halo_send.at[1], halo_recv.at[1], (me, left)
        )
        fields_right = remote(
            fields.at[:, :, last_own, :], fields.at[:, :, low_rows, :],
            field_send.at[0], field_recv.at[0], (me, right),
        )
        fields_left = remote(
            fields.at[:, :, first_own, :], fields.at[:, :, high_rows, :],
            field_send.at[1], field_recv.at[1], (me, left),
        )
        mixed_right = remote(
            mixed.at[:, :, last_own, :], mixed.at[:, :, low_rows, :],
            mixed_send.at[0], mixed_recv.at[0], (me, right),
        )
        mixed_left = remote(
            mixed.at[:, :, first_own, :], mixed.at[:, :, high_rows, :],
            mixed_send.at[1], mixed_recv.at[1], (me, left),
        )

        tap_weight = [weights[s] for s in range(TAPS)]
        along = [offsets[0, s] for s in range(TAPS)]
        across = [offsets[1, s] for s in range(TAPS)]

        def mix(source, at, k):
            for half in range(halves):
                total = None
                for level in range(levels):
                    term = source[level, k, :, half * LANES : (half + 1) * LANES].astype(F32) * z[
                        level * halves + half, at, :
                    ]
                    total = term if total is None else total + term
                mixed[k, half, at, :] = total

        def mix_own():
            def step(k, carry):
                for more in range(UNROLL):
                    mix(p, own, UNROLL * k + more)
                return carry

            lax.fori_loop(0, members // UNROLL, step, 0)

        def mix_edges():
            def step(k, carry):
                for more in range(UNROLL):
                    mix(p_low, low_rows, UNROLL * k + more)
                    mix(p_high, high_rows, UNROLL * k + more)
                return carry

            lax.fori_loop(0, members // UNROLL, step, 0)

        reach = width + 2 * RADIUS
        row_at = lax.broadcasted_iota(jnp.int32, (reach, LANES), 0) + (col * width - RADIUS)
        keep = jnp.where((row_at >= 0) & (row_at < blocks * width), 1.0, 0.0)

        def turns(amounts):
            spots = [lax.broadcasted_iota(jnp.int32, (1, LANES), 1) - v for v in amounts]
            return (
                [jnp.where(v < 0, v + LANES, v) for v in amounts],
                [(s >= 0) & (s < LANES) for s in spots],
            )

        back, forth = turns(across), turns([-v for v in across])

        def stencil(source, starts, count, moves):
            total = [None] * halves
            for s in range(TAPS):
                turned = [
                    pltpu.roll(source(half, pl.ds(starts[s], count)), moves[0][s], 1)
                    for half in range(halves)
                ]
                for half in range(halves):
                    term = tap_weight[s] * jnp.where(
                        moves[1][s], turned[half], turned[1 - half]
                    )
                    total[half] = term if total[half] is None else total[half] + term
            return total

        def transpose_taps(turn):
            starts = [RADIUS - v for v in along]

            def step(k, carry):
                for more in range(TAP_UNROLL):
                    at = TAP_UNROLL * k + more
                    total = stencil(lambda h, rows_at: mixed[at, h, rows_at, :], starts, reach, back)
                    for half in range(halves):
                        resid[turn, at, half, pl.ds(RADIUS, reach), :] = total[half] * keep
                return carry

            lax.fori_loop(0, members // TAP_UNROLL, step, 0)

        def taps_and_sum(turn):
            starts = [HALO + v for v in along]

            def step(k, so_far):
                for more in range(TAP_UNROLL):
                    at = TAP_UNROLL * k + more
                    total = stencil(
                        lambda h, rows_at: resid[turn, at, h, rows_at, :], starts, width, forth
                    )
                    so_far = tuple(
                        so_far[level * halves + half]
                        + p[level, at, :, half * LANES : (half + 1) * LANES].astype(F32) * total[half]
                        for level in range(levels)
                        for half in range(halves)
                    )
                return so_far

            summed = lax.fori_loop(
                0,
                members // TAP_UNROLL,
                step,
                tuple(jnp.zeros((width, LANES), F32) for _ in range(planes)),
            )
            for plane in range(planes):
                part[turn, plane] = summed[plane]

        def chunk_copy(turn, step):
            peer = lax.rem(me + step, groups)
            return remote(
                part.at[turn, peer], gathered.at[turn, step - 1],
                rs_send.at[turn, step - 1], rs_recv.at[turn, step - 1], (peer, col),
            )

        def whole_copy(turn, step, sender, peer):
            spot = full.at[turn, sender, own, :]
            return remote(
                spot, spot, ag_send.at[turn, step - 1], ag_recv.at[turn, step - 1], (peer, col)
            )

        def edge_copies(turn, other, sender, slot):
            return (
                remote(
                    full.at[turn, sender, last_own, :], full.at[turn, sender, low_rows, :],
                    low_send.at[turn, other], low_recv.at[turn, slot], (other, right),
                ),
                remote(
                    full.at[turn, sender, first_own, :], full.at[turn, sender, high_rows, :],
                    high_send.at[turn, other], high_recv.at[turn, slot], (other, left),
                ),
            )

        def note_copy(which, step, sender, peer):
            return remote(
                note.at[which], group_note.at[which, sender],
                note_send.at[which, step - 1], note_recv.at[which, step - 1], (peer, col),
            )

        def sum_copy(which, step, sender, peer):
            return remote(
                sums.at[which], block_note.at[which, sender],
                sum_send.at[which, step - 1], sum_recv.at[which, step - 1], (me, peer),
            )

        def start_sums(turn):
            def step(s, carry):
                chunk_copy(turn, s).start()
                return carry

            lax.fori_loop(1, groups, step, 0)

        def finish_sums(turn):
            def step(s, carry):
                chunk_copy(turn, s).wait_recv()
                return carry

            lax.fori_loop(1, groups, step, 0)
            total = part[turn, me]
            for s in range(groups - 1):
                total = total + gathered[turn, s]
            full[turn, me, own, :] = total
            return total

        def start_spread(turn, edges):
            if edges:

                def edge_step(other, carry):
                    for copy in edge_copies(turn, other, me, me):
                        copy.start()
                    return carry

                lax.fori_loop(0, groups, edge_step, 0)

            def step(s, carry):
                whole_copy(turn, s, me, lax.rem(me + s, groups)).start()
                return carry

            lax.fori_loop(1, groups, step, 0)

        def finish_own(turn):
            def step(s, carry):
                peer = lax.rem(me + groups - s, groups)
                whole_copy(turn, s, peer, peer).wait_recv()
                return carry

            lax.fori_loop(1, groups, step, 0)

        def finish_edges(turn):
            def step(other, carry):
                for copy in edge_copies(turn, other, other, other):
                    copy.wait_recv()
                return carry

            lax.fori_loop(0, groups, step, 0)

        def send_note(which, values):
            row = jnp.zeros((1, LANES), F32)
            for at, value in enumerate(values):
                row = jnp.where(lanes8 == at, value, row)
            note[which] = row
            group_note[which, me] = row

            def step(s, carry):
                note_copy(which, s, me, lax.rem(me + s, groups)).start()
                return carry

            lax.fori_loop(1, groups, step, 0)

        def pass_note(which):
            def step(s, carry):
                peer = lax.rem(me + groups - s, groups)
                note_copy(which, s, peer, peer).wait_recv()
                return carry

            lax.fori_loop(1, groups, step, 0)
            total = group_note[which, 0]
            for other in range(1, groups):
                total = total + group_note[which, other]
            sums[which] = total
            block_note[which, col] = total

            def send(s, carry):
                sum_copy(which, s, col, lax.rem(col + s, blocks)).start()
                return carry

            lax.fori_loop(1, blocks, send, 0)

        def read_note(which, count):
            def step(s, carry):
                peer = lax.rem(col + blocks - s, blocks)
                sum_copy(which, s, peer, peer).wait_recv()
                return carry

            lax.fori_loop(1, blocks, step, 0)
            total = block_note[which, 0]
            for other in range(1, blocks):
                total = total + block_note[which, other]
            return [
                jnp.sum(jnp.where(lanes8 == at, total, 0.0), axis=1, keepdims=True)
                for at in range(count)
            ]

        def out_copies(which):
            source = (resid.at[0, :, :, own, :], second, resid.at[2, :, :, own, :])[which]
            target = (out_a, out_b, out_c)[which]
            return [
                pltpu.make_async_copy(
                    source.at[:, half],
                    target.at[:, :, pl.ds(half * LANES, LANES)],
                    out_sem.at[which, half],
                )
                for half in range(halves)
            ]

        def store_out(which):
            for copy in out_copies(which):
                copy.start()

        def all_of(value):
            return jnp.sum(jnp.sum(value, axis=0, keepdims=True), axis=1, keepdims=True)

        load.wait()
        for plane in range(planes):
            z[plane, own, :] = fields[0, plane, own, :]
        mix_own()
        pl.semaphore_wait(barrier, groups - 1 + 2 * groups + blocks - 1)
        mixed_right.start()
        mixed_left.start()
        mixed_right.wait_recv()
        mixed_left.wait_recv()
        for copy in (fields_right, fields_left, to_right, to_left):
            copy.start()

        @pl.when(col == 0)
        def _():
            mixed[:, :, low_rows, :] = jnp.zeros((members, halves, HALO, LANES), F32)

        @pl.when(col == blocks - 1)
        def _():
            mixed[:, :, high_rows, :] = jnp.zeros((members, halves, HALO, LANES), F32)

        transpose_taps(0)
        taps_and_sum(0)
        start_sums(0)
        store_out(0)

        def square(k, total):
            for half in range(halves):
                value = resid[0, k, half, own, :]
                total = total + value * value
            return total

        norm = all_of(lax.fori_loop(0, members, square, jnp.zeros((width, LANES), F32)))
        mine = finish_sums(0)
        start_spread(0, True)
        send_note(0, [norm, all_of(fields[1, me, own, :] * mine * mine)])
        finish_own(0)
        pass_note(0)

        def image_of_first(at):
            for plane in range(planes):
                z[plane, at, :] = (
                    fields[0, plane, at, :] + fields[1, plane, at, :] * full[0, plane, at, :]
                )

        mixed_right.wait_send()
        mixed_left.wait_send()
        image_of_first(own)
        mix_own()
        fields_right.wait_recv()
        fields_left.wait_recv()
        has_left = jnp.where(col > 0, 1.0, 0.0)
        has_right = jnp.where(col < blocks - 1, 1.0, 0.0)
        for which in range(2):
            for plane in range(planes):
                fields[which, plane, low_rows, :] = fields[which, plane, low_rows, :] * has_left
                fields[which, plane, high_rows, :] = fields[which, plane, high_rows, :] * has_right
        finish_edges(0)
        to_right.wait_recv()
        to_left.wait_recv()
        image_of_first(low_rows)
        image_of_first(high_rows)
        mix_edges()
        transpose_taps(1)
        taps_and_sum(1)
        start_sums(1)
        finish_sums(1)
        start_spread(1, True)
        norm_0, bend_0 = read_note(0, 2)
        curve_0 = norm_0 + bend_0
        step_0 = norm_0 / curve_0
        finish_own(1)

        def image_of_second(at):
            for plane in range(planes):
                z[plane, at, :] = (fields[0, plane, at, :] - step_0 * z[plane, at, :]) + fields[
                    1, plane, at, :
                ] * (full[0, plane, at, :] - step_0 * full[1, plane, at, :])

        image_of_second(own)
        mix_own()
        finish_edges(1)
        image_of_second(low_rows)
        image_of_second(high_rows)
        mix_edges()
        transpose_taps(2)
        taps_and_sum(2)
        start_sums(2)
        store_out(2)

        def products(k, so_far):
            ab, ac, bb, bc, cc = so_far
            for half in range(halves):
                a = resid[0, k, half, own, :]
                b = a - step_0 * resid[1, k, half, own, :]
                c = resid[2, k, half, own, :]
                second[k, half] = b
                ab, ac, bb, bc, cc = ab + a * b, ac + a * c, bb + b * b, bc + b * c, cc + c * c
            return ab, ac, bb, bc, cc

        inner = [
            all_of(v)
            for v in lax.fori_loop(
                0, members, products, tuple(jnp.zeros((width, LANES), F32) for _ in range(5))
            )
        ]
        store_out(1)
        mine_c = finish_sums(2)
        start_spread(2, False)
        mine_a = full[0, me, own, :]
        mine_b = mine_a - step_0 * full[1, me, own, :]
        weight = fields[1, me, own, :]
        wb, wc = weight * mine_b, weight * mine_c
        bends = [all_of(v) for v in (wb * mine_a, wc * mine_a, wb * mine_b, wc * mine_b, wc * mine_c)]
        send_note(1, inner + bends)
        pass_note(1)
        g_ab, g_ac, g_bb, g_bc, g_cc, e_ab, e_ac, e_bb, e_bc, e_cc = read_note(1, 10)
        finish_own(2)

        def form(aa, ab, ac, bb, bc, cc, u):
            a, b, c = u
            return (
                a * a * aa + b * b * bb + c * c * cc + 2.0 * (a * b * ab + a * c * ac + b * c * bc)
            )

        h = (curve_0, g_ab + e_ab, g_ac + e_ac, g_bb + e_bb, g_bc + e_bc, g_cc + e_cc)
        one = jnp.ones_like(norm_0)
        ratio_0 = g_bb / norm_0
        d1 = (ratio_0, one, 0.0 * one)
        step_1 = g_bb / form(*h, d1)
        mixing = step_1 * ratio_0 / step_0
        r2 = (-mixing, one + mixing, -step_1)
        norm_2 = form(norm_0, g_ab, g_ac, g_bb, g_bc, g_cc, r2)
        ratio_1 = norm_2 / g_bb
        d2 = tuple(r + ratio_1 * d for r, d in zip(r2, d1))
        step_2 = norm_2 / form(*h, d2)
        in_a = step_0 + step_1 * d1[0] + step_2 * d2[0]
        in_b = step_1 * d1[1] + step_2 * d2[1]
        in_c = step_1 * d1[2] + step_2 * d2[2]

        for at, value in enumerate((in_a, in_b, in_c)):
            coefficients[pl.ds(at, 1), :] = jnp.broadcast_to(value, (1, depth))
        for level in range(levels):
            for half in range(halves):
                plane = level * halves + half
                at = (level, slice(None), slice(half * LANES, (half + 1) * LANES))
                a = full[0, plane, own, :]
                inc_a[at] = a
                inc_b[at] = a - step_0 * full[1, plane, own, :]
                inc_c[at] = full[2, plane, own, :]

        for copy in (to_right, to_left, fields_right, fields_left):
            copy.wait_send()
        for which in range(3):
            for copy in out_copies(which):
                copy.wait()
        for turn in range(3):

            def settle(s, carry):
                chunk_copy(turn, s).wait_send()
                whole_copy(turn, s, me, lax.rem(me + s, groups)).wait_send()
                return carry

            lax.fori_loop(1, groups, settle, 0)
        for turn in range(2):

            def settle_edges(other, carry):
                for copy in edge_copies(turn, other, me, me):
                    copy.wait_send()
                return carry

            lax.fori_loop(0, groups, settle_edges, 0)

            def settle_notes(s, carry):
                note_copy(turn, s, me, lax.rem(me + s, groups)).wait_send()
                return carry

            lax.fori_loop(1, groups, settle_notes, 0)

            def settle_blocks(s, carry):
                sum_copy(turn, s, col, lax.rem(col + s, blocks)).wait_send()
                return carry

            lax.fori_loop(1, blocks, settle_blocks, 0)

    bf16 = jnp.bfloat16
    dma = pltpu.SemaphoreType.DMA
    scratch = [
        pltpu.VMEM((levels, members, width, depth), bf16),
        pltpu.VMEM((levels, members, HALO, depth), bf16),
        pltpu.VMEM((levels, members, HALO, depth), bf16),
        pltpu.VMEM((2, planes, rows, LANES), F32),
        pltpu.VMEM((planes, rows, LANES), F32),
        pltpu.VMEM((members, halves, rows, LANES), F32),
        pltpu.VMEM((3, members, halves, rows, LANES), F32),
        pltpu.VMEM((members, halves, width, LANES), F32),
        pltpu.VMEM((3, planes, width, LANES), F32),
        pltpu.VMEM((3, groups - 1, width, LANES), F32),
        pltpu.VMEM((3, planes, rows, LANES), F32),
        pltpu.VMEM((2, 1, LANES), F32),
        pltpu.VMEM((2, groups, 1, LANES), F32),
        pltpu.VMEM((2, 1, LANES), F32),
        pltpu.VMEM((2, blocks, 1, LANES), F32),
        dma,
        dma((3, halves)), dma((2,)), dma((2,)), dma((2,)), dma((2,)), dma((2,)), dma((2,)),
        dma((3, groups - 1)), dma((3, groups - 1)), dma((3, groups - 1)), dma((3, groups - 1)),
        dma((2, groups)), dma((2, groups)), dma((2, groups)), dma((2, groups)),
        dma((2, groups - 1)), dma((2, groups - 1)), dma((2, blocks - 1)), dma((2, blocks - 1)),
    ]
    return kernel, scratch


def solution(mesh):
    groups, blocks = mesh.shape["mem"], mesh.shape["col"]

    def per_device(perturbations, loc_weights, offsets, obs_x, obs_y, obs_t, innovations, obs_rinv):
        levels, members, width, depth = perturbations.shape
        obs_rows = obs_x.shape[0] // LANES
        kernel, scratch = make_kernel(groups, blocks, levels, members, width, depth, obs_rows)
        vmem = pl.BlockSpec(memory_space=pltpu.VMEM)
        smem = pl.BlockSpec(memory_space=pltpu.SMEM)
        hbm = pl.BlockSpec(memory_space=pl.ANY)
        a, b, c, inc_a, inc_b, inc_c, factors = pl.pallas_call(
            kernel,
            out_shape=(jax.ShapeDtypeStruct((members, width, depth), F32),) * 3
            + (jax.ShapeDtypeStruct((levels, width, depth), F32),) * 3
            + (jax.ShapeDtypeStruct((3, depth), F32),),
            in_specs=[hbm, smem, smem] + [vmem] * 5,
            out_specs=(hbm,) * 3 + (vmem,) * 4,
            scratch_shapes=scratch,
            compiler_params=pltpu.CompilerParams(collective_id=0, has_side_effects=True),
        )(
            perturbations, loc_weights, offsets.T,
            *(v.reshape(obs_rows, LANES) for v in (obs_x, obs_y, obs_t, innovations, obs_rinv)),
        )
        return (
            factors[0] * a + factors[1] * b + factors[2] * c,
            factors[0] * inc_a + factors[1] * inc_b + factors[2] * inc_c,
        )

    return jax.shard_map(
        per_device,
        mesh=mesh,
        in_specs=(P(None, "mem", "col", None), P(), P()) + (P("col"),) * 5,
        out_specs=(P("mem", "col", None), P(None, "col", None)),
        check_vma=False,
    )
```

```python
import jax
import jax.numpy as jnp
from jax import lax
from jax.experimental import pallas as pl
from jax.experimental.pallas import tpu as pltpu
from jax.sharding import PartitionSpec as P

TAPS = 7
RADIUS = 4
LANES = 128
HALO = 2 * RADIUS
F32 = jnp.float32
UNROLL = 4
TAP_UNROLL = 4
MESH = pl.DeviceIdType.MESH


def make_kernel(groups, blocks, levels, members, width, depth, obs_rows):
    halves = depth // LANES
    planes = levels * halves
    rows = width + 2 * HALO
    own = pl.ds(HALO, width)
    low_rows = pl.ds(0, HALO)
    high_rows = pl.ds(HALO + width, HALO)
    last_own = pl.ds(width, HALO)
    first_own = pl.ds(HALO, HALO)

    def kernel(
        pert, weights, offsets, obs_x, obs_y, obs_t, innov, rinv,
        control, increment,
        p, p_low, p_high, fields, z, mixed, resid, second, part, gathered, full,
        note, group_note, sums, block_note,
        hello, load_sem, mixed_send, mixed_recv, halo_send, halo_recv, field_send, field_recv,
        rs_send, rs_recv, ag_send, ag_recv, low_send, low_recv, high_send, high_recv,
        note_send, note_recv, sum_send, sum_recv,
    ):
        me = lax.axis_index("mem")
        col = lax.axis_index("col")
        right = lax.rem(col + 1, blocks)
        left = lax.rem(col + blocks - 1, blocks)

        barrier = pltpu.get_barrier_semaphore()

        def greet(target):
            pl.semaphore_signal(barrier, inc=1, device_id=target, device_id_type=MESH)

        load = pltpu.make_async_copy(pert, p, load_sem)
        load.start()
        for step in range(1, groups):
            greet((lax.rem(me + step, groups), col))
        greet((me, right))
        greet((me, left))

        def hello_peers(turn):
            away = 1 << turn
            return lax.rem(col + away, blocks), lax.rem(col + blocks - away, blocks)

        def say_hello(turn):
            up, down = hello_peers(turn)
            pl.semaphore_signal(hello.at[turn, 0], inc=1, device_id=(me, up), device_id_type=MESH)
            pl.semaphore_signal(hello.at[turn, 1], inc=1, device_id=(me, down), device_id_type=MESH)

        def hear_hello(turn):
            pl.semaphore_wait(hello.at[turn, 0], 1)
            pl.semaphore_wait(hello.at[turn, 1], 1)

        lanes8 = lax.broadcasted_iota(jnp.int32, (1, LANES), 1)
        cell_rows = lax.broadcasted_iota(jnp.int32, (levels * width, LANES), 0)
        depth_rows = lax.broadcasted_iota(jnp.int32, (depth, LANES), 0)

        def place(chunk, total):
            at = pl.ds(chunk, 1)
            cell = obs_t[at, :] * width + (obs_x[at, :] - col * width)
            r = rinv[at, :]
            hit = cell_rows == cell
            pieces = []
            for value in (r * innov[at, :], r):
                rest = value
                for _ in range(3):
                    piece = rest.astype(jnp.bfloat16)
                    rest = rest - piece.astype(F32)
                    pieces.append(jnp.where(hit, piece.astype(F32), 0.0).astype(jnp.bfloat16))
            left_side = jnp.concatenate(pieces, axis=0)
            right_side = jnp.where(depth_rows == obs_y[at, :], 1.0, 0.0).astype(jnp.bfloat16)
            return total + lax.dot_general(
                left_side, right_side, (((1,), (1,)), ((), ())), preferred_element_type=F32
            )

        spread = lax.fori_loop(
            0, obs_rows, place, jnp.zeros((6 * levels * width, depth), F32)
        )
        cells = levels * width
        for which in range(2):
            base = 3 * which * cells
            summed = (
                spread[base : base + cells]
                + spread[base + cells : base + 2 * cells]
                + spread[base + 2 * cells : base + 3 * cells]
            )
            for level in range(levels):
                for half in range(halves):
                    fields[which, level * halves + half, own, :] = summed[
                        level * width : (level + 1) * width, half * LANES : (half + 1) * LANES
                    ]

        def remote(source, target, send, recv, device):
            return pltpu.make_async_remote_copy(
                src_ref=source, dst_ref=target, send_sem=send, recv_sem=recv,
                device_id=device, device_id_type=MESH,
            )

        to_right = remote(
            pert.at[:, :, pl.ds(width - HALO, HALO), :], p_low, halo_send.at[0], halo_recv.at[0], (me, right)
        )
        to_left = remote(
            pert.at[:, :, pl.ds(0, HALO), :], p_high, halo_send.at[1], halo_recv.at[1], (me, left)
        )
        fields_right = remote(
            fields.at[:, :, last_own, :], fields.at[:, :, low_rows, :],
            field_send.at[0], field_recv.at[0], (me, right),
        )
        fields_left = remote(
            fields.at[:, :, first_own, :], fields.at[:, :, high_rows, :],
            field_send.at[1], field_recv.at[1], (me, left),
        )
        mixed_right = remote(
            mixed.at[:, :, last_own, :], mixed.at[:, :, low_rows, :],
            mixed_send.at[0], mixed_recv.at[0], (me, right),
        )
        mixed_left = remote(
            mixed.at[:, :, first_own, :], mixed.at[:, :, high_rows, :],
            mixed_send.at[1], mixed_recv.at[1], (me, left),
        )

        tap_weight = [weights[s] for s in range(TAPS)]
        along = [offsets[0, s] for s in range(TAPS)]
        across = [offsets[1, s] for s in range(TAPS)]

        def mix(source, at, k):
            for half in range(halves):
                total = None
                for level in range(levels):
                    term = source[level, k, :, half * LANES : (half + 1) * LANES].astype(F32) * z[
                        level * halves + half, at, :
                    ]
                    total = term if total is None else total + term
                mixed[k, half, at, :] = total

        def mix_own():
            def step(k, carry):
                for more in range(UNROLL):
                    mix(p, own, UNROLL * k + more)
                return carry

            lax.fori_loop(0, members // UNROLL, step, 0)

        def mix_edges():
            def step(k, carry):
                for more in range(UNROLL):
                    mix(p_low, low_rows, UNROLL * k + more)
                    mix(p_high, high_rows, UNROLL * k + more)
                return carry

            lax.fori_loop(0, members // UNROLL, step, 0)

        reach = width + 2 * RADIUS
        row_at = lax.broadcasted_iota(jnp.int32, (reach, LANES), 0) + (col * width - RADIUS)
        keep = jnp.where((row_at >= 0) & (row_at < blocks * width), 1.0, 0.0)

        def turns(amounts):
            spots = [lax.broadcasted_iota(jnp.int32, (1, LANES), 1) - v for v in amounts]
            return (
                [jnp.where(v < 0, v + LANES, v) for v in amounts],
                [(s >= 0) & (s < LANES) for s in spots],
            )

        back, forth = turns(across), turns([-v for v in across])

        def stencil(source, starts, count, moves):
            total = [None] * halves
            for s in range(TAPS):
                turned = [
                    pltpu.roll(source(half, pl.ds(starts[s], count)), moves[0][s], 1)
                    for half in range(halves)
                ]
                for half in range(halves):
                    term = tap_weight[s] * jnp.where(
                        moves[1][s], turned[half], turned[1 - half]
                    )
                    total[half] = term if total[half] is None else total[half] + term
            return total

        def transpose_taps(turn):
            starts = [RADIUS - v for v in along]

            def step(k, carry):
                for more in range(TAP_UNROLL):
                    at = TAP_UNROLL * k + more
                    total = stencil(lambda h, rows_at: mixed[at, h, rows_at, :], starts, reach, back)
                    for half in range(halves):
                        resid[turn, at, half, pl.ds(RADIUS, reach), :] = total[half] * keep
                return carry

            lax.fori_loop(0, members // TAP_UNROLL, step, 0)

        def taps_and_sum(turn):
            starts = [HALO + v for v in along]

            def step(k, so_far):
                for more in range(TAP_UNROLL):
                    at = TAP_UNROLL * k + more
                    total = stencil(
                        lambda h, rows_at: resid[turn, at, h, rows_at, :], starts, width, forth
                    )
                    so_far = tuple(
                        so_far[level * halves + half]
                        + p[level, at, :, half * LANES : (half + 1) * LANES].astype(F32) * total[half]
                        for level in range(levels)
                        for half in range(halves)
                    )
                return so_far

            summed = lax.fori_loop(
                0,
                members // TAP_UNROLL,
                step,
                tuple(jnp.zeros((width, LANES), F32) for _ in range(planes)),
            )
            for plane in range(planes):
                part[turn, plane] = summed[plane]

        def chunk_copy(turn, step):
            peer = lax.rem(me + step, groups)
            return remote(
                part.at[turn, peer], gathered.at[turn, step - 1],
                rs_send.at[turn, step - 1], rs_recv.at[turn, step - 1], (peer, col),
            )

        def whole_copy(turn, step, sender, peer):
            spot = full.at[turn, sender, own, :]
            return remote(
                spot, spot, ag_send.at[turn, step - 1], ag_recv.at[turn, step - 1], (peer, col)
            )

        def edge_copies(turn, other, sender, slot):
            return (
                remote(
                    full.at[turn, sender, last_own, :], full.at[turn, sender, low_rows, :],
                    low_send.at[turn, other], low_recv.at[turn, slot], (other, right),
                ),
                remote(
                    full.at[turn, sender, first_own, :], full.at[turn, sender, high_rows, :],
                    high_send.at[turn, other], high_recv.at[turn, slot], (other, left),
                ),
            )

        def note_copy(which, step, sender, peer):
            return remote(
                note.at[which], group_note.at[which, sender],
                note_send.at[which, step - 1], note_recv.at[which, step - 1], (peer, col),
            )

        def sum_copy(which, step, sender, peer):
            return remote(
                sums.at[which], block_note.at[which, sender],
                sum_send.at[which, step - 1], sum_recv.at[which, step - 1], (me, peer),
            )

        def start_sums(turn):
            def step(s, carry):
                chunk_copy(turn, s).start()
                return carry

            lax.fori_loop(1, groups, step, 0)

        def finish_sums(turn):
            def step(s, carry):
                chunk_copy(turn, s).wait_recv()
                return carry

            lax.fori_loop(1, groups, step, 0)
            total = part[turn, me]
            for s in range(groups - 1):
                total = total + gathered[turn, s]
            full[turn, me, own, :] = total
            return total

        def start_spread(turn, edges):
            if edges:

                def edge_step(other, carry):
                    for copy in edge_copies(turn, other, me, me):
                        copy.start()
                    return carry

                lax.fori_loop(0, groups, edge_step, 0)

            def step(s, carry):
                whole_copy(turn, s, me, lax.rem(me + s, groups)).start()
                return carry

            lax.fori_loop(1, groups, step, 0)

        def finish_own(turn):
            def step(s, carry):
                peer = lax.rem(me + groups - s, groups)
                whole_copy(turn, s, peer, peer).wait_recv()
                return carry

            lax.fori_loop(1, groups, step, 0)

        def finish_edges(turn):
            def step(other, carry):
                for copy in edge_copies(turn, other, other, other):
                    copy.wait_recv()
                return carry

            lax.fori_loop(0, groups, step, 0)

        def send_note(which, values):
            row = jnp.zeros((1, LANES), F32)
            for at, value in enumerate(values):
                row = jnp.where(lanes8 == at, value, row)
            note[which] = row
            group_note[which, me] = row

            def step(s, carry):
                note_copy(which, s, me, lax.rem(me + s, groups)).start()
                return carry

            lax.fori_loop(1, groups, step, 0)

        def pass_note(which):
            def step(s, carry):
                peer = lax.rem(me + groups - s, groups)
                note_copy(which, s, peer, peer).wait_recv()
                return carry

            lax.fori_loop(1, groups, step, 0)
            total = group_note[which, 0]
            for other in range(1, groups):
                total = total + group_note[which, other]
            sums[which] = total
            block_note[which, col] = total

            def send(s, carry):
                sum_copy(which, s, col, lax.rem(col + s, blocks)).start()
                return carry

            lax.fori_loop(1, blocks, send, 0)

        def read_note(which, count):
            def step(s, carry):
                peer = lax.rem(col + blocks - s, blocks)
                sum_copy(which, s, peer, peer).wait_recv()
                return carry

            lax.fori_loop(1, blocks, step, 0)
            total = block_note[which, 0]
            for other in range(1, blocks):
                total = total + block_note[which, other]
            return [
                jnp.sum(jnp.where(lanes8 == at, total, 0.0), axis=1, keepdims=True)
                for at in range(count)
            ]

        def all_of(value):
            return jnp.sum(jnp.sum(value, axis=0, keepdims=True), axis=1, keepdims=True)

        load.wait()
        for plane in range(planes):
            z[plane, own, :] = fields[0, plane, own, :]
        mix_own()
        pl.semaphore_wait(barrier, groups - 1 + 2)
        mixed_right.start()
        mixed_left.start()
        for copy in (fields_right, fields_left, to_right, to_left):
            copy.start()
        say_hello(0)
        mixed_right.wait_recv()
        mixed_left.wait_recv()
        hear_hello(0)
        say_hello(1)

        @pl.when(col == 0)
        def _():
            mixed[:, :, low_rows, :] = jnp.zeros((members, halves, HALO, LANES), F32)

        @pl.when(col == blocks - 1)
        def _():
            mixed[:, :, high_rows, :] = jnp.zeros((members, halves, HALO, LANES), F32)

        transpose_taps(0)
        hear_hello(1)
        say_hello(2)
        taps_and_sum(0)
        start_sums(0)

        def square(k, total):
            for half in range(halves):
                value = resid[0, k, half, own, :]
                total = total + value * value
            return total

        norm = all_of(lax.fori_loop(0, members, square, jnp.zeros((width, LANES), F32)))
        mine = finish_sums(0)
        hear_hello(2)
        say_hello(3)
        start_spread(0, True)
        send_note(0, [norm, all_of(fields[1, me, own, :] * mine * mine)])
        finish_own(0)
        hear_hello(3)
        pass_note(0)

        def image_of_first(at):
            for plane in range(planes):
                z[plane, at, :] = (
                    fields[0, plane, at, :] + fields[1, plane, at, :] * full[0, plane, at, :]
                )

        mixed_right.wait_send()
        mixed_left.wait_send()
        image_of_first(own)
        mix_own()
        fields_right.wait_recv()
        fields_left.wait_recv()
        has_left = jnp.where(col > 0, 1.0, 0.0)
        has_right = jnp.where(col < blocks - 1, 1.0, 0.0)
        for which in range(2):
            for plane in range(planes):
                fields[which, plane, low_rows, :] = fields[which, plane, low_rows, :] * has_left
                fields[which, plane, high_rows, :] = fields[which, plane, high_rows, :] * has_right
        finish_edges(0)
        to_right.wait_recv()
        to_left.wait_recv()
        image_of_first(low_rows)
        image_of_first(high_rows)
        mix_edges()
        transpose_taps(1)
        taps_and_sum(1)
        start_sums(1)
        finish_sums(1)
        start_spread(1, True)
        norm_0, bend_0 = read_note(0, 2)
        curve_0 = norm_0 + bend_0
        step_0 = norm_0 / curve_0
        finish_own(1)

        def image_of_second(at):
            for plane in range(planes):
                z[plane, at, :] = (fields[0, plane, at, :] - step_0 * z[plane, at, :]) + fields[
                    1, plane, at, :
                ] * (full[0, plane, at, :] - step_0 * full[1, plane, at, :])

        image_of_second(own)
        mix_own()
        finish_edges(1)
        image_of_second(low_rows)
        image_of_second(high_rows)
        mix_edges()
        transpose_taps(2)
        taps_and_sum(2)
        start_sums(2)

        def products(k, so_far):
            ab, ac, bb, bc, cc = so_far
            for half in range(halves):
                a = resid[0, k, half, own, :]
                b = a - step_0 * resid[1, k, half, own, :]
                c = resid[2, k, half, own, :]
                second[k, half] = b
                ab, ac, bb, bc, cc = ab + a * b, ac + a * c, bb + b * b, bc + b * c, cc + c * c
            return ab, ac, bb, bc, cc

        inner = [
            all_of(v)
            for v in lax.fori_loop(
                0, members, products, tuple(jnp.zeros((width, LANES), F32) for _ in range(5))
            )
        ]
        mine_c = finish_sums(2)
        start_spread(2, False)
        mine_a = full[0, me, own, :]
        mine_b = mine_a - step_0 * full[1, me, own, :]
        weight = fields[1, me, own, :]
        wb, wc = weight * mine_b, weight * mine_c
        bends = [all_of(v) for v in (wb * mine_a, wc * mine_a, wb * mine_b, wc * mine_b, wc * mine_c)]
        send_note(1, inner + bends)
        pass_note(1)
        g_ab, g_ac, g_bb, g_bc, g_cc, e_ab, e_ac, e_bb, e_bc, e_cc = read_note(1, 10)
        finish_own(2)

        def form(aa, ab, ac, bb, bc, cc, u):
            a, b, c = u
            return (
                a * a * aa + b * b * bb + c * c * cc + 2.0 * (a * b * ab + a * c * ac + b * c * bc)
            )

        h = (curve_0, g_ab + e_ab, g_ac + e_ac, g_bb + e_bb, g_bc + e_bc, g_cc + e_cc)
        one = jnp.ones_like(norm_0)
        ratio_0 = g_bb / norm_0
        d1 = (ratio_0, one, 0.0 * one)
        step_1 = g_bb / form(*h, d1)
        mixing = step_1 * ratio_0 / step_0
        r2 = (-mixing, one + mixing, -step_1)
        norm_2 = form(norm_0, g_ab, g_ac, g_bb, g_bc, g_cc, r2)
        ratio_1 = norm_2 / g_bb
        d2 = tuple(r + ratio_1 * d for r, d in zip(r2, d1))
        step_2 = norm_2 / form(*h, d2)
        in_a = step_0 + step_1 * d1[0] + step_2 * d2[0]
        in_b = step_1 * d1[1] + step_2 * d2[1]
        in_c = step_1 * d1[2] + step_2 * d2[2]

        def write(step, carry):
            for more in range(UNROLL):
                k = UNROLL * step + more
                for half in range(halves):
                    control[k, :, half * LANES : (half + 1) * LANES] = (
                        in_a * resid[0, k, half, own, :]
                        + in_b * second[k, half]
                        + in_c * resid[2, k, half, own, :]
                    )
            return carry

        lax.fori_loop(0, members // UNROLL, write, 0)
        for level in range(levels):
            for half in range(halves):
                plane = level * halves + half
                a = full[0, plane, own, :]
                b = a - step_0 * full[1, plane, own, :]
                increment[level, :, half * LANES : (half + 1) * LANES] = (
                    in_a * a + in_b * b + in_c * full[2, plane, own, :]
                )

        for copy in (to_right, to_left, fields_right, fields_left):
            copy.wait_send()
        for turn in range(3):

            def settle(s, carry):
                chunk_copy(turn, s).wait_send()
                whole_copy(turn, s, me, lax.rem(me + s, groups)).wait_send()
                return carry

            lax.fori_loop(1, groups, settle, 0)
        for turn in range(2):

            def settle_edges(other, carry):
                for copy in edge_copies(turn, other, me, me):
                    copy.wait_send()
                return carry

            lax.fori_loop(0, groups, settle_edges, 0)

            def settle_notes(s, carry):
                note_copy(turn, s, me, lax.rem(me + s, groups)).wait_send()
                return carry

            lax.fori_loop(1, groups, settle_notes, 0)

            def settle_blocks(s, carry):
                sum_copy(turn, s, col, lax.rem(col + s, blocks)).wait_send()
                return carry

            lax.fori_loop(1, blocks, settle_blocks, 0)

    bf16 = jnp.bfloat16
    dma = pltpu.SemaphoreType.DMA
    scratch = [
        pltpu.VMEM((levels, members, width, depth), bf16),
        pltpu.VMEM((levels, members, HALO, depth), bf16),
        pltpu.VMEM((levels, members, HALO, depth), bf16),
        pltpu.VMEM((2, planes, rows, LANES), F32),
        pltpu.VMEM((planes, rows, LANES), F32),
        pltpu.VMEM((members, halves, rows, LANES), F32),
        pltpu.VMEM((3, members, halves, rows, LANES), F32),
        pltpu.VMEM((members, halves, width, LANES), F32),
        pltpu.VMEM((3, planes, width, LANES), F32),
        pltpu.VMEM((3, groups - 1, width, LANES), F32),
        pltpu.VMEM((3, planes, rows, LANES), F32),
        pltpu.VMEM((2, 1, LANES), F32),
        pltpu.VMEM((2, groups, 1, LANES), F32),
        pltpu.VMEM((2, 1, LANES), F32),
        pltpu.VMEM((2, blocks, 1, LANES), F32),
        pltpu.SemaphoreType.REGULAR((4, 2)),
        dma,
        dma((2,)), dma((2,)), dma((2,)), dma((2,)), dma((2,)), dma((2,)),
        dma((3, groups - 1)), dma((3, groups - 1)), dma((3, groups - 1)), dma((3, groups - 1)),
        dma((2, groups)), dma((2, groups)), dma((2, groups)), dma((2, groups)),
        dma((2, groups - 1)), dma((2, groups - 1)), dma((2, blocks - 1)), dma((2, blocks - 1)),
    ]
    return kernel, scratch


def solution(mesh):
    groups, blocks = mesh.shape["mem"], mesh.shape["col"]

    def per_device(perturbations, loc_weights, offsets, obs_x, obs_y, obs_t, innovations, obs_rinv):
        levels, members, width, depth = perturbations.shape
        obs_rows = obs_x.shape[0] // LANES
        kernel, scratch = make_kernel(groups, blocks, levels, members, width, depth, obs_rows)
        vmem = pl.BlockSpec(memory_space=pltpu.VMEM)
        smem = pl.BlockSpec(memory_space=pltpu.SMEM)
        hbm = pl.BlockSpec(memory_space=pl.ANY)
        return pl.pallas_call(
            kernel,
            out_shape=(
                pltpu.VMEM((members, width, depth), F32),
                pltpu.VMEM((levels, width, depth), F32),
            ),
            in_specs=[hbm, smem, smem] + [vmem] * 5,
            out_specs=(vmem,) * 2,
            scratch_shapes=scratch,
            compiler_params=pltpu.CompilerParams(collective_id=0, has_side_effects=True),
        )(
            perturbations, loc_weights, offsets.T,
            *(v.reshape(obs_rows, LANES) for v in (obs_x, obs_y, obs_t, innovations, obs_rinv)),
        )

    return jax.shard_map(
        per_device,
        mesh=mesh,
        in_specs=(P(None, "mem", "col", None), P(), P()) + (P("col"),) * 5,
        out_specs=(P("mem", "col", None), P(None, "col", None)),
        check_vma=False,
    )
```

```python
import jax
import jax.numpy as jnp
from jax import lax
from jax.experimental import pallas as pl
from jax.experimental.pallas import tpu as pltpu
from jax.sharding import PartitionSpec as P

TAPS = 7
RADIUS = 4
LANES = 128
HALO = 2 * RADIUS
F32 = jnp.float32
UNROLL = 4
TAP_UNROLL = 4
MESH = pl.DeviceIdType.MESH


def make_kernel(groups, blocks, levels, members, width, depth, obs_rows):
    halves = depth // LANES
    planes = levels * halves
    rows = width + 2 * HALO
    own = pl.ds(HALO, width)
    low_rows = pl.ds(0, HALO)
    high_rows = pl.ds(HALO + width, HALO)
    last_own = pl.ds(width, HALO)
    first_own = pl.ds(HALO, HALO)

    def kernel(
        pert, weights_in, offsets_in, obs_x_in, obs_y_in, obs_t_in, innov_in, rinv_in,
        control, increment,
        weights, offsets, obs_x, obs_y, obs_t, innov, rinv,
        p, p_low, p_high, fields, z, mixed, resid, second, part, gathered, full,
        note, group_note, sums, block_note,
        hello, load_sem, mixed_send, mixed_recv, halo_send, halo_recv, field_send, field_recv,
        rs_send, rs_recv, ag_send, ag_recv, low_send, low_recv, high_send, high_recv,
        note_send, note_recv, sum_send, sum_recv,
    ):
        me = lax.axis_index("mem")
        col = lax.axis_index("col")
        right, left = col + 1, col - 1
        has_left, has_right = col > 0, col < blocks - 1

        barrier = pltpu.get_barrier_semaphore()

        def greet(target):
            pl.semaphore_signal(barrier, inc=1, device_id=target, device_id_type=MESH)

        loads = [
            pltpu.make_async_copy(source, target, load_sem.at[at])
            for at, (source, target) in enumerate(
                (
                    (obs_x_in, obs_x), (obs_y_in, obs_y), (obs_t_in, obs_t), (innov_in, innov),
                    (rinv_in, rinv), (weights_in, weights), (offsets_in, offsets), (pert, p),
                )
            )
        ]
        load = loads.pop()
        for copy in loads:
            copy.start()
        load.start()
        for step in range(1, groups):
            greet((lax.rem(me + step, groups), col))

        @pl.when(has_right)
        def _():
            greet((me, right))

        @pl.when(has_left)
        def _():
            greet((me, left))

        def hello_sides(turn):
            away = 1 << turn
            return (0, col + away, col + away < blocks), (1, col - away, col >= away)

        def say_hello(turn):
            for side, peer, there in hello_sides(turn):

                @pl.when(there)
                def _():
                    pl.semaphore_signal(
                        hello.at[turn, side], inc=1, device_id=(me, peer), device_id_type=MESH
                    )

        def hear_hello(turn):
            for side, _, there in hello_sides(turn):

                @pl.when(there)
                def _():
                    pl.semaphore_wait(hello.at[turn, 1 - side], 1)

        @pl.when(col == 0)
        def _():
            p_low[...] = jnp.zeros(p_low.shape, p_low.dtype)
            fields[:, :, low_rows, :] = jnp.zeros((2, planes, HALO, LANES), F32)
            full[:, :, low_rows, :] = jnp.zeros((3, planes, HALO, LANES), F32)

        @pl.when(col == blocks - 1)
        def _():
            p_high[...] = jnp.zeros(p_high.shape, p_high.dtype)
            fields[:, :, high_rows, :] = jnp.zeros((2, planes, HALO, LANES), F32)
            full[:, :, high_rows, :] = jnp.zeros((3, planes, HALO, LANES), F32)

        lanes8 = lax.broadcasted_iota(jnp.int32, (1, LANES), 1)
        cell_rows = lax.broadcasted_iota(jnp.int32, (levels * width, LANES), 0)
        depth_rows = lax.broadcasted_iota(jnp.int32, (depth, LANES), 0)

        def place(chunk, total):
            at = pl.ds(chunk, 1)
            cell = obs_t[at, :] * width + (obs_x[at, :] - col * width)
            r = rinv[at, :]
            hit = cell_rows == cell
            pieces = []
            for value in (r * innov[at, :], r):
                rest = value
                for _ in range(3):
                    piece = rest.astype(jnp.bfloat16)
                    rest = rest - piece.astype(F32)
                    pieces.append(jnp.where(hit, piece.astype(F32), 0.0).astype(jnp.bfloat16))
            left_side = jnp.concatenate(pieces, axis=0)
            right_side = jnp.where(depth_rows == obs_y[at, :], 1.0, 0.0).astype(jnp.bfloat16)
            return total + lax.dot_general(
                left_side, right_side, (((1,), (1,)), ((), ())), preferred_element_type=F32
            )

        for copy in loads:
            copy.wait()
        spread = lax.fori_loop(
            0, obs_rows, place, jnp.zeros((6 * levels * width, depth), F32)
        )
        cells = levels * width
        for which in range(2):
            base = 3 * which * cells
            summed = (
                spread[base : base + cells]
                + spread[base + cells : base + 2 * cells]
                + spread[base + 2 * cells : base + 3 * cells]
            )
            for level in range(levels):
                for half in range(halves):
                    fields[which, level * halves + half, own, :] = summed[
                        level * width : (level + 1) * width, half * LANES : (half + 1) * LANES
                    ]

        def remote(source, target, send, recv, device):
            return pltpu.make_async_remote_copy(
                src_ref=source, dst_ref=target, send_sem=send, recv_sem=recv,
                device_id=device, device_id_type=MESH,
            )

        to_right = [
            remote(
                pert.at[level, :, pl.ds(width - HALO, HALO), :], p_low.at[level],
                halo_send.at[0, level], halo_recv.at[0, level], (me, right),
            )
            for level in range(levels)
        ]
        to_left = [
            remote(
                pert.at[level, :, pl.ds(0, HALO), :], p_high.at[level],
                halo_send.at[1, level], halo_recv.at[1, level], (me, left),
            )
            for level in range(levels)
        ]

        def send_halo(*which):
            @pl.when(has_right)
            def _():
                for level in which:
                    to_right[level].start()

            @pl.when(has_left)
            def _():
                for level in which:
                    to_left[level].start()

        fields_right = remote(
            fields.at[:, :, last_own, :], fields.at[:, :, low_rows, :],
            field_send.at[0], field_recv.at[0], (me, right),
        )
        fields_left = remote(
            fields.at[:, :, first_own, :], fields.at[:, :, high_rows, :],
            field_send.at[1], field_recv.at[1], (me, left),
        )
        mixed_right = remote(
            mixed.at[:, :, last_own, :], mixed.at[:, :, low_rows, :],
            mixed_send.at[0], mixed_recv.at[0], (me, right),
        )
        mixed_left = remote(
            mixed.at[:, :, first_own, :], mixed.at[:, :, high_rows, :],
            mixed_send.at[1], mixed_recv.at[1], (me, left),
        )

        tap_weight = [weights[s] for s in range(TAPS)]
        along = [offsets[0, s] for s in range(TAPS)]
        across = [offsets[1, s] for s in range(TAPS)]

        def mix(source, at, k):
            for half in range(halves):
                total = None
                for level in range(levels):
                    term = source[level, k, :, half * LANES : (half + 1) * LANES].astype(F32) * z[
                        level * halves + half, at, :
                    ]
                    total = term if total is None else total + term
                mixed[k, half, at, :] = total

        def mix_own():
            def step(k, carry):
                for more in range(UNROLL):
                    mix(p, own, UNROLL * k + more)
                return carry

            lax.fori_loop(0, members // UNROLL, step, 0)

        def mix_edges():
            def step(k, carry):
                for more in range(UNROLL):
                    mix(p_low, low_rows, UNROLL * k + more)
                    mix(p_high, high_rows, UNROLL * k + more)
                return carry

            lax.fori_loop(0, members // UNROLL, step, 0)

        reach = width + 2 * RADIUS
        row_at = lax.broadcasted_iota(jnp.int32, (reach, LANES), 0) + (col * width - RADIUS)
        keep = jnp.where((row_at >= 0) & (row_at < blocks * width), 1.0, 0.0)

        def turns(amounts):
            spots = [lax.broadcasted_iota(jnp.int32, (1, LANES), 1) - v for v in amounts]
            return (
                [jnp.where(v < 0, v + LANES, v) for v in amounts],
                [(s >= 0) & (s < LANES) for s in spots],
            )

        back, forth = turns(across), turns([-v for v in across])

        def stencil(source, starts, count, moves):
            total = [None] * halves
            for s in range(TAPS):
                turned = [
                    pltpu.roll(source(half, pl.ds(starts[s], count)), moves[0][s], 1)
                    for half in range(halves)
                ]
                for half in range(halves):
                    term = tap_weight[s] * jnp.where(
                        moves[1][s], turned[half], turned[1 - half]
                    )
                    total[half] = term if total[half] is None else total[half] + term
            return total

        def transpose_taps(turn):
            starts = [RADIUS - v for v in along]

            def step(k, carry):
                for more in range(TAP_UNROLL):
                    at = TAP_UNROLL * k + more
                    total = stencil(lambda h, rows_at: mixed[at, h, rows_at, :], starts, reach, back)
                    for half in range(halves):
                        resid[turn, at, half, pl.ds(RADIUS, reach), :] = total[half] * keep
                return carry

            lax.fori_loop(0, members // TAP_UNROLL, step, 0)

        def taps_and_sum(turn):
            starts = [HALO + v for v in along]

            def step(k, so_far):
                for more in range(TAP_UNROLL):
                    at = TAP_UNROLL * k + more
                    total = stencil(
                        lambda h, rows_at: resid[turn, at, h, rows_at, :], starts, width, forth
                    )
                    so_far = tuple(
                        so_far[level * halves + half]
                        + p[level, at, :, half * LANES : (half + 1) * LANES].astype(F32) * total[half]
                        for level in range(levels)
                        for half in range(halves)
                    )
                return so_far

            summed = lax.fori_loop(
                0,
                members // TAP_UNROLL,
                step,
                tuple(jnp.zeros((width, LANES), F32) for _ in range(planes)),
            )
            for plane in range(planes):
                part[turn, plane] = summed[plane]

        def wait_bytes(ref, sem):
            pltpu.make_async_copy(ref, ref, sem).wait()

        def start_sums(turn):
            for step in range(1, groups):
                peer = lax.rem(me + step, groups)
                remote(
                    part.at[turn, peer], gathered.at[turn, step - 1],
                    rs_send.at[turn], rs_recv.at[turn], (peer, col),
                ).start()

        def finish_sums(turn):
            wait_bytes(gathered.at[turn], rs_recv.at[turn])
            total = part[turn, me]
            for s in range(groups - 1):
                total = total + gathered[turn, s]
            full[turn, me, own, :] = total
            return total

        def start_edges(turn):
            @pl.when(has_right)
            def _():
                for step in range(groups):
                    remote(
                        full.at[turn, me, last_own, :], full.at[turn, me, low_rows, :],
                        low_send.at[turn], low_recv.at[turn], (lax.rem(me + step, groups), right),
                    ).start()

            @pl.when(has_left)
            def _():
                for step in range(groups):
                    remote(
                        full.at[turn, me, first_own, :], full.at[turn, me, high_rows, :],
                        high_send.at[turn], high_recv.at[turn], (lax.rem(me + step, groups), left),
                    ).start()

        def start_group(turn):
            spot = full.at[turn, me, own, :]
            for step in range(1, groups):
                remote(
                    spot, spot, ag_send.at[turn], ag_recv.at[turn], (lax.rem(me + step, groups), col)
                ).start()

        def others(turn):
            return full.at[turn, pl.ds(0, groups - 1), own, :]

        def finish_own(turn):
            wait_bytes(others(turn), ag_recv.at[turn])

        def finish_edges(turn):
            @pl.when(has_left)
            def _():
                wait_bytes(full.at[turn, :, low_rows, :], low_recv.at[turn])

            @pl.when(has_right)
            def _():
                wait_bytes(full.at[turn, :, high_rows, :], high_recv.at[turn])

        def send_note(which, values):
            row = jnp.zeros((1, LANES), F32)
            for at, value in enumerate(values):
                row = jnp.where(lanes8 == at, value, row)
            note[which] = row
            group_note[which, me] = row
            for step in range(1, groups):
                remote(
                    note.at[which], group_note.at[which, me],
                    note_send.at[which], note_recv.at[which], (lax.rem(me + step, groups), col),
                ).start()

        def pass_note(which):
            wait_bytes(group_note.at[which, pl.ds(0, groups - 1)], note_recv.at[which])
            total = group_note[which, 0]
            for other in range(1, groups):
                total = total + group_note[which, other]
            sums[which] = total
            block_note[which, col] = total
            for step in range(1, blocks):
                remote(
                    sums.at[which], block_note.at[which, col],
                    sum_send.at[which], sum_recv.at[which], (me, lax.rem(col + step, blocks)),
                ).start()

        def read_note(which, count):
            wait_bytes(block_note.at[which, pl.ds(0, blocks - 1)], sum_recv.at[which])
            total = block_note[which, 0]
            for other in range(1, blocks):
                total = total + block_note[which, other]
            return [
                jnp.sum(jnp.where(lanes8 == at, total, 0.0), axis=1, keepdims=True)
                for at in range(count)
            ]

        def all_of(value):
            return jnp.sum(jnp.sum(value, axis=0, keepdims=True), axis=1, keepdims=True)

        load.wait()
        for plane in range(planes):
            z[plane, own, :] = fields[0, plane, own, :]
        mix_own()
        beside = lax.div(col + blocks - 1, blocks) + lax.div(2 * blocks - 2 - col, blocks)
        pl.semaphore_wait(barrier, groups - 1 + beside)

        @pl.when(has_right)
        def _():
            mixed_right.start()
            fields_right.start()

        @pl.when(has_left)
        def _():
            mixed_left.start()
            fields_left.start()

        send_halo(0)
        say_hello(0)

        @pl.when(has_left)
        def _():
            mixed_right.wait_recv()

        @pl.when(has_right)
        def _():
            mixed_left.wait_recv()

        hear_hello(0)
        say_hello(1)

        @pl.when(col == 0)
        def _():
            mixed[:, :, low_rows, :] = jnp.zeros((members, halves, HALO, LANES), F32)

        @pl.when(col == blocks - 1)
        def _():
            mixed[:, :, high_rows, :] = jnp.zeros((members, halves, HALO, LANES), F32)

        transpose_taps(0)
        hear_hello(1)
        say_hello(2)
        taps_and_sum(0)
        hear_hello(2)
        say_hello(3)
        start_sums(0)
        send_halo(1, 2)

        def square(k, total):
            for half in range(halves):
                value = resid[0, k, half, own, :]
                total = total + value * value
            return total

        norm = all_of(lax.fori_loop(0, members, square, jnp.zeros((width, LANES), F32)))
        mine = finish_sums(0)
        hear_hello(3)
        say_hello(4)
        start_edges(0)
        start_group(0)
        send_halo(3)
        send_note(0, [norm, all_of(fields[1, me, own, :] * mine * mine)])
        finish_own(0)

        def image_of_first(at):
            for plane in range(planes):
                z[plane, at, :] = (
                    fields[0, plane, at, :] + fields[1, plane, at, :] * full[0, plane, at, :]
                )


        @pl.when(has_right)
        def _():
            mixed_right.wait_send()

        @pl.when(has_left)
        def _():
            mixed_left.wait_send()

        image_of_first(own)
        mix_own()
        hear_hello(4)
        pass_note(0)
        finish_edges(0)

        @pl.when(has_left)
        def _():
            fields_right.wait_recv()
            for copy in to_right:
                copy.wait_recv()

        @pl.when(has_right)
        def _():
            fields_left.wait_recv()
            for copy in to_left:
                copy.wait_recv()

        image_of_first(low_rows)
        image_of_first(high_rows)
        mix_edges()
        transpose_taps(1)
        taps_and_sum(1)
        start_sums(1)
        finish_sums(1)
        start_edges(1)
        start_group(1)
        norm_0, bend_0 = read_note(0, 2)
        curve_0 = norm_0 + bend_0
        step_0 = norm_0 / curve_0
        finish_own(1)

        def image_of_second(at):
            for plane in range(planes):
                z[plane, at, :] = (fields[0, plane, at, :] - step_0 * z[plane, at, :]) + fields[
                    1, plane, at, :
                ] * (full[0, plane, at, :] - step_0 * full[1, plane, at, :])

        image_of_second(own)
        mix_own()
        finish_edges(1)
        image_of_second(low_rows)
        image_of_second(high_rows)
        mix_edges()
        transpose_taps(2)
        taps_and_sum(2)
        start_sums(2)

        def products(k, so_far):
            ab, ac, bb, bc, cc = so_far
            for half in range(halves):
                a = resid[0, k, half, own, :]
                b = a - step_0 * resid[1, k, half, own, :]
                c = resid[2, k, half, own, :]
                second[k, half] = b
                ab, ac, bb, bc, cc = ab + a * b, ac + a * c, bb + b * b, bc + b * c, cc + c * c
            return ab, ac, bb, bc, cc

        inner = [
            all_of(v)
            for v in lax.fori_loop(
                0, members, products, tuple(jnp.zeros((width, LANES), F32) for _ in range(5))
            )
        ]
        mine_c = finish_sums(2)
        mine_a = full[0, me, own, :]
        mine_b = mine_a - step_0 * full[1, me, own, :]
        weight = fields[1, me, own, :]
        wb, wc = weight * mine_b, weight * mine_c
        bends = [all_of(v) for v in (wb * mine_a, wc * mine_a, wb * mine_b, wc * mine_b, wc * mine_c)]
        send_note(1, inner + bends)
        start_group(2)
        pass_note(1)
        g_ab, g_ac, g_bb, g_bc, g_cc, e_ab, e_ac, e_bb, e_bc, e_cc = read_note(1, 10)
        finish_own(2)

        def form(aa, ab, ac, bb, bc, cc, u):
            a, b, c = u
            return (
                a * a * aa + b * b * bb + c * c * cc + 2.0 * (a * b * ab + a * c * ac + b * c * bc)
            )

        h = (curve_0, g_ab + e_ab, g_ac + e_ac, g_bb + e_bb, g_bc + e_bc, g_cc + e_cc)
        one = jnp.ones_like(norm_0)
        ratio_0 = g_bb / norm_0
        d1 = (ratio_0, one, 0.0 * one)
        step_1 = g_bb / form(*h, d1)
        mixing = step_1 * ratio_0 / step_0
        r2 = (-mixing, one + mixing, -step_1)
        norm_2 = form(norm_0, g_ab, g_ac, g_bb, g_bc, g_cc, r2)
        ratio_1 = norm_2 / g_bb
        d2 = tuple(r + ratio_1 * d for r, d in zip(r2, d1))
        step_2 = norm_2 / form(*h, d2)
        in_a = step_0 + step_1 * d1[0] + step_2 * d2[0]
        in_b = step_1 * d1[1] + step_2 * d2[1]
        in_c = step_1 * d1[2] + step_2 * d2[2]

        def write(step, carry):
            for more in range(UNROLL):
                k = UNROLL * step + more
                for half in range(halves):
                    control[k, :, half * LANES : (half + 1) * LANES] = (
                        in_a * resid[0, k, half, own, :]
                        + in_b * second[k, half]
                        + in_c * resid[2, k, half, own, :]
                    )
            return carry

        lax.fori_loop(0, members // UNROLL, write, 0)
        for level in range(levels):
            for half in range(halves):
                plane = level * halves + half
                a = full[0, plane, own, :]
                b = a - step_0 * full[1, plane, own, :]
                increment[level, :, half * LANES : (half + 1) * LANES] = (
                    in_a * a + in_b * b + in_c * full[2, plane, own, :]
                )

        @pl.when(has_right)
        def _():
            for copy in to_right:
                copy.wait_send()
            fields_right.wait_send()

        @pl.when(has_left)
        def _():
            for copy in to_left:
                copy.wait_send()
            fields_left.wait_send()

        for turn in range(3):
            wait_bytes(gathered.at[turn], rs_send.at[turn])
            wait_bytes(others(turn), ag_send.at[turn])
        for turn in range(2):

            @pl.when(has_right)
            def _():
                wait_bytes(full.at[turn, :, low_rows, :], low_send.at[turn])

            @pl.when(has_left)
            def _():
                wait_bytes(full.at[turn, :, high_rows, :], high_send.at[turn])

            wait_bytes(group_note.at[turn, pl.ds(0, groups - 1)], note_send.at[turn])
            wait_bytes(block_note.at[turn, pl.ds(0, blocks - 1)], sum_send.at[turn])

    bf16 = jnp.bfloat16
    dma = pltpu.SemaphoreType.DMA
    scratch = [
        pltpu.SMEM((TAPS,), F32),
        pltpu.SMEM((2, TAPS), jnp.int32),
        pltpu.VMEM((obs_rows, LANES), jnp.int32),
        pltpu.VMEM((obs_rows, LANES), jnp.int32),
        pltpu.VMEM((obs_rows, LANES), jnp.int32),
        pltpu.VMEM((obs_rows, LANES), F32),
        pltpu.VMEM((obs_rows, LANES), F32),
        pltpu.VMEM((levels, members, width, depth), bf16),
        pltpu.VMEM((levels, members, HALO, depth), bf16),
        pltpu.VMEM((levels, members, HALO, depth), bf16),
        pltpu.VMEM((2, planes, rows, LANES), F32),
        pltpu.VMEM((planes, rows, LANES), F32),
        pltpu.VMEM((members, halves, rows, LANES), F32),
        pltpu.VMEM((3, members, halves, rows, LANES), F32),
        pltpu.VMEM((members, halves, width, LANES), F32),
        pltpu.VMEM((3, planes, width, LANES), F32),
        pltpu.VMEM((3, groups - 1, width, LANES), F32),
        pltpu.VMEM((3, planes, rows, LANES), F32),
        pltpu.VMEM((2, 1, LANES), F32),
        pltpu.VMEM((2, groups, 1, LANES), F32),
        pltpu.VMEM((2, 1, LANES), F32),
        pltpu.VMEM((2, blocks, 1, LANES), F32),
        pltpu.SemaphoreType.REGULAR((5, 2)),
        dma((8,)),
        dma((2,)), dma((2,)), dma((2, levels)), dma((2, levels)), dma((2,)), dma((2,)),
        dma((3,)), dma((3,)), dma((3,)), dma((3,)),
        dma((2,)), dma((2,)), dma((2,)), dma((2,)),
        dma((2,)), dma((2,)), dma((2,)), dma((2,)),
    ]
    return kernel, scratch


def solution(mesh):
    groups, blocks = mesh.shape["mem"], mesh.shape["col"]

    def per_device(perturbations, loc_weights, offsets, obs_x, obs_y, obs_t, innovations, obs_rinv):
        levels, members, width, depth = perturbations.shape
        obs_rows = obs_x.shape[0] // LANES
        kernel, scratch = make_kernel(groups, blocks, levels, members, width, depth, obs_rows)
        vmem = pl.BlockSpec(memory_space=pltpu.VMEM)
        hbm = pl.BlockSpec(memory_space=pl.ANY)
        return pl.pallas_call(
            kernel,
            out_shape=(
                pltpu.VMEM((members, width, depth), F32),
                pltpu.VMEM((levels, width, depth), F32),
            ),
            in_specs=[hbm] * 8,
            out_specs=(vmem,) * 2,
            scratch_shapes=scratch,
            compiler_params=pltpu.CompilerParams(collective_id=0, has_side_effects=True),
        )(
            perturbations, loc_weights, offsets.T,
            *(v.reshape(obs_rows, LANES) for v in (obs_x, obs_y, obs_t, innovations, obs_rinv)),
        )

    return jax.shard_map(
        per_device,
        mesh=mesh,
        in_specs=(P(None, "mem", "col", None), P(), P()) + (P("col"),) * 5,
        out_specs=(P("mem", "col", None), P(None, "col", None)),
        check_vma=False,
    )
```

```python
import jax
import jax.numpy as jnp
from jax import lax
from jax.experimental import pallas as pl
from jax.experimental.pallas import tpu as pltpu
from jax.sharding import PartitionSpec as P

TAPS = 7
RADIUS = 4
LANES = 128
HALO = 2 * RADIUS
F32 = jnp.float32
UNROLL = 4
CHUNK = 8
MESH = pl.DeviceIdType.MESH


def make_kernel(groups, blocks, levels, members, width, depth, obs_rows):
    halves = depth // LANES
    planes = levels * halves
    rows = width + 2 * HALO
    chunks = members // CHUNK
    own = pl.ds(HALO, width)
    low_rows = pl.ds(0, HALO)
    high_rows = pl.ds(HALO + width, HALO)
    last_own = pl.ds(width, HALO)
    first_own = pl.ds(HALO, HALO)

    def kernel(
        pert, weights_in, offsets_in, obs_x_in, obs_y_in, obs_t_in, innov_in, rinv_in,
        control, increment,
        weights, offsets, obs_x, obs_y, obs_t, innov, rinv,
        p, p_low, p_high, p_right, p_left, mix_out, mix_in, fields, z, mixed, resid, second, part, gathered, full,
        note, group_note, sums, block_note,
        hello, load_sem, mixed_send, mixed_recv, halo_send, halo_recv, field_send, field_recv,
        rs_send, rs_recv, ag_send, ag_recv, low_send, low_recv, high_send, high_recv,
        note_send, note_recv, sum_send, sum_recv,
    ):
        me = lax.axis_index("mem")
        col = lax.axis_index("col")
        right, left = col + 1, col - 1
        has_left, has_right = col > 0, col < blocks - 1

        barrier = pltpu.get_barrier_semaphore()

        def greet(target):
            pl.semaphore_signal(barrier, inc=1, device_id=target, device_id_type=MESH)

        loads = [
            pltpu.make_async_copy(source, target, load_sem.at[at])
            for at, (source, target) in enumerate(
                (
                    (obs_x_in, obs_x), (obs_y_in, obs_y), (obs_t_in, obs_t), (innov_in, innov),
                    (rinv_in, rinv), (weights_in, weights), (offsets_in, offsets), (pert, p),
                    (pert.at[:, :, pl.ds(width - HALO, HALO), :], p_right),
                    (pert.at[:, :, pl.ds(0, HALO), :], p_left),
                )
            )
        ]
        for copy in loads:
            copy.start()
        edge_loads, load, loads = loads[-2:], loads[-3], loads[:-3]
        for step in range(1, groups):
            greet((lax.rem(me + step, groups), col))

        @pl.when(has_right)
        def _():
            greet((me, right))

        @pl.when(has_left)
        def _():
            greet((me, left))

        def hello_sides(turn):
            away = 1 << turn
            return (0, col + away, col + away < blocks), (1, col - away, col >= away)

        def say_hello(turn):
            for side, peer, there in hello_sides(turn):

                @pl.when(there)
                def _():
                    pl.semaphore_signal(
                        hello.at[turn, side], inc=1, device_id=(me, peer), device_id_type=MESH
                    )

        def hear_hello(turn):
            for side, _, there in hello_sides(turn):

                @pl.when(there)
                def _():
                    pl.semaphore_wait(hello.at[turn, 1 - side], 1)

        @pl.when(col == 0)
        def _():
            p_low[...] = jnp.zeros(p_low.shape, p_low.dtype)
            mix_in[0] = jnp.zeros((members, halves, HALO, LANES), F32)
            fields[:, :, low_rows, :] = jnp.zeros((2, planes, HALO, LANES), F32)
            full[:, :, low_rows, :] = jnp.zeros((3, planes, HALO, LANES), F32)

        @pl.when(col == blocks - 1)
        def _():
            p_high[...] = jnp.zeros(p_high.shape, p_high.dtype)
            mix_in[1] = jnp.zeros((members, halves, HALO, LANES), F32)
            fields[:, :, high_rows, :] = jnp.zeros((2, planes, HALO, LANES), F32)
            full[:, :, high_rows, :] = jnp.zeros((3, planes, HALO, LANES), F32)

        lanes8 = lax.broadcasted_iota(jnp.int32, (1, LANES), 1)
        cell_rows = lax.broadcasted_iota(jnp.int32, (levels * width, LANES), 0)
        depth_rows = lax.broadcasted_iota(jnp.int32, (depth, LANES), 0)

        def place(chunk, total):
            at = pl.ds(chunk, 1)
            cell = obs_t[at, :] * width + (obs_x[at, :] - col * width)
            r = rinv[at, :]
            hit = cell_rows == cell
            pieces = []
            for value in (r * innov[at, :], r):
                rest = value
                for _ in range(3):
                    piece = rest.astype(jnp.bfloat16)
                    rest = rest - piece.astype(F32)
                    pieces.append(jnp.where(hit, piece.astype(F32), 0.0).astype(jnp.bfloat16))
            left_side = jnp.concatenate(pieces, axis=0)
            right_side = jnp.where(depth_rows == obs_y[at, :], 1.0, 0.0).astype(jnp.bfloat16)
            return total + lax.dot_general(
                left_side, right_side, (((1,), (1,)), ((), ())), preferred_element_type=F32
            )

        for copy in loads:
            copy.wait()
        spread = lax.fori_loop(
            0, obs_rows, place, jnp.zeros((6 * levels * width, depth), F32)
        )
        cells = levels * width
        for which in range(2):
            base = 3 * which * cells
            summed = (
                spread[base : base + cells]
                + spread[base + cells : base + 2 * cells]
                + spread[base + 2 * cells : base + 3 * cells]
            )
            for level in range(levels):
                for half in range(halves):
                    fields[which, level * halves + half, own, :] = summed[
                        level * width : (level + 1) * width, half * LANES : (half + 1) * LANES
                    ]

        def remote(source, target, send, recv, device):
            return pltpu.make_async_remote_copy(
                src_ref=source, dst_ref=target, send_sem=send, recv_sem=recv,
                device_id=device, device_id_type=MESH,
            )

        def members_of(chunk):
            return pl.ds(chunk * CHUNK, CHUNK)

        def to_right(chunk):
            return remote(
                p_right.at[:, members_of(chunk)], p_low.at[:, members_of(chunk)],
                halo_send.at[0, chunk], halo_recv.at[0, chunk], (me, right),
            )

        def to_left(chunk):
            return remote(
                p_left.at[:, members_of(chunk)], p_high.at[:, members_of(chunk)],
                halo_send.at[1, chunk], halo_recv.at[1, chunk], (me, left),
            )

        def mixed_right(chunk):
            return remote(
                mix_out.at[0, members_of(chunk)], mix_in.at[0, members_of(chunk)],
                mixed_send.at[0, chunk], mixed_recv.at[0, chunk], (me, right),
            )

        def mixed_left(chunk):
            return remote(
                mix_out.at[1, members_of(chunk)], mix_in.at[1, members_of(chunk)],
                mixed_send.at[1, chunk], mixed_recv.at[1, chunk], (me, left),
            )

        def send_halo(*which):
            @pl.when(has_right)
            def _():
                for chunk in which:
                    to_right(chunk).start()

            @pl.when(has_left)
            def _():
                for chunk in which:
                    to_left(chunk).start()

        fields_right = remote(
            fields.at[:, :, last_own, :], fields.at[:, :, low_rows, :],
            field_send.at[0], field_recv.at[0], (me, right),
        )
        fields_left = remote(
            fields.at[:, :, first_own, :], fields.at[:, :, high_rows, :],
            field_send.at[1], field_recv.at[1], (me, left),
        )
        tap_weight = [weights[s] for s in range(TAPS)]
        along = [offsets[0, s] for s in range(TAPS)]
        across = [offsets[1, s] for s in range(TAPS)]

        def mix(source, at, k, out=False):
            for half in range(halves):
                total = None
                for level in range(levels):
                    term = source[level, k, :, half * LANES : (half + 1) * LANES].astype(F32) * z[
                        level * halves + half, at, :
                    ]
                    total = term if total is None else total + term
                mixed[k, half, at, :] = total
                if out:
                    mix_out[0, k, half] = total[width - HALO :]
                    mix_out[1, k, half] = total[:HALO]

        def mix_own(out=False):
            def step(k, carry):
                for more in range(UNROLL):
                    mix(p, own, UNROLL * k + more, out)
                return carry

            lax.fori_loop(0, members // UNROLL, step, 0)

        reach = width + 2 * RADIUS
        row_at = lax.broadcasted_iota(jnp.int32, (reach, LANES), 0) + (col * width - RADIUS)
        keep = jnp.where((row_at >= 0) & (row_at < blocks * width), 1.0, 0.0)

        def turns(amounts):
            spots = [lax.broadcasted_iota(jnp.int32, (1, LANES), 1) - v for v in amounts]
            return (
                [jnp.where(v < 0, v + LANES, v) for v in amounts],
                [(s >= 0) & (s < LANES) for s in spots],
            )

        back, forth = turns(across), turns([-v for v in across])

        def stencil(source, starts, count, moves):
            total = [None] * halves
            for s in range(TAPS):
                turned = [
                    pltpu.roll(source(half, pl.ds(starts[s], count)), moves[0][s], 1)
                    for half in range(halves)
                ]
                for half in range(halves):
                    term = tap_weight[s] * jnp.where(
                        moves[1][s], turned[half], turned[1 - half]
                    )
                    total[half] = term if total[half] is None else total[half] + term
            return total

        back_starts = [RADIUS - v for v in along]
        forth_starts = [HALO + v for v in along]

        def first_edges(chunk):
            pl.when(has_left)(lambda: mixed_right(chunk).wait_recv())
            pl.when(has_right)(lambda: mixed_left(chunk).wait_recv())
            for more in range(CHUNK):
                k = CHUNK * chunk + more
                for half in range(halves):
                    mixed[k, half, low_rows, :] = mix_in[0, k, half]
                    mixed[k, half, high_rows, :] = mix_in[1, k, half]

        def later_edges(chunk):
            for more in range(CHUNK):
                mix(p_low, low_rows, CHUNK * chunk + more)
                mix(p_high, high_rows, CHUNK * chunk + more)

        def arriving_edges(chunk):
            pl.when(has_left)(lambda: to_right(chunk).wait_recv())
            pl.when(has_right)(lambda: to_left(chunk).wait_recv())
            later_edges(chunk)

        def apply(turn, edges):
            def step(chunk, so_far):
                edges(chunk)
                for more in range(CHUNK):
                    k = CHUNK * chunk + more
                    total = stencil(lambda h, rows_at: mixed[k, h, rows_at, :], back_starts, reach, back)
                    for half in range(halves):
                        resid[turn, k, half, pl.ds(RADIUS, reach), :] = total[half] * keep
                for more in range(CHUNK):
                    k = CHUNK * chunk + more
                    total = stencil(
                        lambda h, rows_at: resid[turn, k, h, rows_at, :], forth_starts, width, forth
                    )
                    so_far = tuple(
                        so_far[level * halves + half]
                        + p[level, k, :, half * LANES : (half + 1) * LANES].astype(F32) * total[half]
                        for level in range(levels)
                        for half in range(halves)
                    )
                return so_far

            summed = lax.fori_loop(
                0, chunks, step, tuple(jnp.zeros((width, LANES), F32) for _ in range(planes))
            )
            for plane in range(planes):
                part[turn, plane] = summed[plane]

        def wait_bytes(ref, sem):
            pltpu.make_async_copy(ref, ref, sem).wait()

        def start_sums(turn):
            for step in range(1, groups):
                peer = lax.rem(me + step, groups)
                remote(
                    part.at[turn, peer], gathered.at[turn, step - 1],
                    rs_send.at[turn], rs_recv.at[turn], (peer, col),
                ).start()

        def finish_sums(turn):
            wait_bytes(gathered.at[turn], rs_recv.at[turn])
            total = part[turn, me]
            for s in range(groups - 1):
                total = total + gathered[turn, s]
            full[turn, me, own, :] = total
            return total

        def start_edges(turn):
            @pl.when(has_right)
            def _():
                for step in range(groups):
                    remote(
                        full.at[turn, me, last_own, :], full.at[turn, me, low_rows, :],
                        low_send.at[turn], low_recv.at[turn], (lax.rem(me + step, groups), right),
                    ).start()

            @pl.when(has_left)
            def _():
                for step in range(groups):
                    remote(
                        full.at[turn, me, first_own, :], full.at[turn, me, high_rows, :],
                        high_send.at[turn], high_recv.at[turn], (lax.rem(me + step, groups), left),
                    ).start()

        def start_group(turn):
            spot = full.at[turn, me, own, :]
            for step in range(1, groups):
                remote(
                    spot, spot, ag_send.at[turn], ag_recv.at[turn], (lax.rem(me + step, groups), col)
                ).start()

        def others(turn):
            return full.at[turn, pl.ds(0, groups - 1), own, :]

        def finish_own(turn):
            wait_bytes(others(turn), ag_recv.at[turn])

        def finish_edges(turn):
            @pl.when(has_left)
            def _():
                wait_bytes(full.at[turn, :, low_rows, :], low_recv.at[turn])

            @pl.when(has_right)
            def _():
                wait_bytes(full.at[turn, :, high_rows, :], high_recv.at[turn])

        def send_note(which, values):
            row = jnp.zeros((1, LANES), F32)
            for at, value in enumerate(values):
                row = jnp.where(lanes8 == at, value, row)
            note[which] = row
            group_note[which, me] = row
            for step in range(1, groups):
                remote(
                    note.at[which], group_note.at[which, me],
                    note_send.at[which], note_recv.at[which], (lax.rem(me + step, groups), col),
                ).start()

        def pass_note(which):
            wait_bytes(group_note.at[which, pl.ds(0, groups - 1)], note_recv.at[which])
            total = group_note[which, 0]
            for other in range(1, groups):
                total = total + group_note[which, other]
            sums[which] = total
            block_note[which, col] = total
            for step in range(1, blocks):
                remote(
                    sums.at[which], block_note.at[which, col],
                    sum_send.at[which], sum_recv.at[which], (me, lax.rem(col + step, blocks)),
                ).start()

        def read_note(which, count):
            wait_bytes(block_note.at[which, pl.ds(0, blocks - 1)], sum_recv.at[which])
            total = block_note[which, 0]
            for other in range(1, blocks):
                total = total + block_note[which, other]
            return [
                jnp.sum(jnp.where(lanes8 == at, total, 0.0), axis=1, keepdims=True)
                for at in range(count)
            ]

        def all_of(value):
            return jnp.sum(jnp.sum(value, axis=0, keepdims=True), axis=1, keepdims=True)

        load.wait()
        for plane in range(planes):
            z[plane, own, :] = fields[0, plane, own, :]
        mix_own(True)
        beside = lax.div(col + blocks - 1, blocks) + lax.div(2 * blocks - 2 - col, blocks)
        pl.semaphore_wait(barrier, groups - 1 + beside)

        @pl.when(has_right)
        def _():
            for chunk in range(chunks):
                mixed_right(chunk).start()
            fields_right.start()

        @pl.when(has_left)
        def _():
            for chunk in range(chunks):
                mixed_left(chunk).start()
            fields_left.start()

        for copy in edge_loads:
            copy.wait()
        send_halo(0)
        say_hello(0)

        hear_hello(0)
        say_hello(1)

        hear_hello(1)
        say_hello(2)
        apply(0, first_edges)
        hear_hello(2)
        say_hello(3)
        start_sums(0)
        send_halo(1, 2)

        def square(k, total):
            for half in range(halves):
                value = resid[0, k, half, own, :]
                total = total + value * value
            return total

        norm = all_of(lax.fori_loop(0, members, square, jnp.zeros((width, LANES), F32)))
        mine = finish_sums(0)
        hear_hello(3)
        say_hello(4)
        start_edges(0)
        start_group(0)
        send_halo(3)
        send_note(0, [norm, all_of(fields[1, me, own, :] * mine * mine)])
        finish_own(0)

        def image_of_first(at):
            for plane in range(planes):
                z[plane, at, :] = (
                    fields[0, plane, at, :] + fields[1, plane, at, :] * full[0, plane, at, :]
                )


        image_of_first(own)
        mix_own()
        hear_hello(4)
        pass_note(0)
        finish_edges(0)

        @pl.when(has_left)
        def _():
            fields_right.wait_recv()

        @pl.when(has_right)
        def _():
            fields_left.wait_recv()

        image_of_first(low_rows)
        image_of_first(high_rows)
        apply(1, arriving_edges)
        start_sums(1)
        finish_sums(1)
        start_edges(1)
        start_group(1)
        norm_0, bend_0 = read_note(0, 2)
        curve_0 = norm_0 + bend_0
        step_0 = norm_0 / curve_0
        finish_own(1)

        def image_of_second(at):
            for plane in range(planes):
                z[plane, at, :] = (fields[0, plane, at, :] - step_0 * z[plane, at, :]) + fields[
                    1, plane, at, :
                ] * (full[0, plane, at, :] - step_0 * full[1, plane, at, :])

        image_of_second(own)
        mix_own()
        finish_edges(1)
        image_of_second(low_rows)
        image_of_second(high_rows)
        apply(2, later_edges)
        start_sums(2)

        def products(k, so_far):
            ab, ac, bb, bc, cc = so_far
            for half in range(halves):
                a = resid[0, k, half, own, :]
                b = a - step_0 * resid[1, k, half, own, :]
                c = resid[2, k, half, own, :]
                second[k, half] = b
                ab, ac, bb, bc, cc = ab + a * b, ac + a * c, bb + b * b, bc + b * c, cc + c * c
            return ab, ac, bb, bc, cc

        inner = [
            all_of(v)
            for v in lax.fori_loop(
                0, members, products, tuple(jnp.zeros((width, LANES), F32) for _ in range(5))
            )
        ]
        mine_c = finish_sums(2)
        mine_a = full[0, me, own, :]
        mine_b = mine_a - step_0 * full[1, me, own, :]
        weight = fields[1, me, own, :]
        wb, wc = weight * mine_b, weight * mine_c
        bends = [all_of(v) for v in (wb * mine_a, wc * mine_a, wb * mine_b, wc * mine_b, wc * mine_c)]
        send_note(1, inner + bends)
        start_group(2)
        pass_note(1)
        g_ab, g_ac, g_bb, g_bc, g_cc, e_ab, e_ac, e_bb, e_bc, e_cc = read_note(1, 10)
        finish_own(2)

        def form(aa, ab, ac, bb, bc, cc, u):
            a, b, c = u
            return (
                a * a * aa + b * b * bb + c * c * cc + 2.0 * (a * b * ab + a * c * ac + b * c * bc)
            )

        h = (curve_0, g_ab + e_ab, g_ac + e_ac, g_bb + e_bb, g_bc + e_bc, g_cc + e_cc)
        one = jnp.ones_like(norm_0)
        ratio_0 = g_bb / norm_0
        d1 = (ratio_0, one, 0.0 * one)
        step_1 = g_bb / form(*h, d1)
        mixing = step_1 * ratio_0 / step_0
        r2 = (-mixing, one + mixing, -step_1)
        norm_2 = form(norm_0, g_ab, g_ac, g_bb, g_bc, g_cc, r2)
        ratio_1 = norm_2 / g_bb
        d2 = tuple(r + ratio_1 * d for r, d in zip(r2, d1))
        step_2 = norm_2 / form(*h, d2)
        in_a = step_0 + step_1 * d1[0] + step_2 * d2[0]
        in_b = step_1 * d1[1] + step_2 * d2[1]
        in_c = step_1 * d1[2] + step_2 * d2[2]

        def write(step, carry):
            for more in range(UNROLL):
                k = UNROLL * step + more
                for half in range(halves):
                    control[k, :, half * LANES : (half + 1) * LANES] = (
                        in_a * resid[0, k, half, own, :]
                        + in_b * second[k, half]
                        + in_c * resid[2, k, half, own, :]
                    )
            return carry

        lax.fori_loop(0, members // UNROLL, write, 0)
        for level in range(levels):
            for half in range(halves):
                plane = level * halves + half
                a = full[0, plane, own, :]
                b = a - step_0 * full[1, plane, own, :]
                increment[level, :, half * LANES : (half + 1) * LANES] = (
                    in_a * a + in_b * b + in_c * full[2, plane, own, :]
                )

        @pl.when(has_right)
        def _():
            fields_right.wait_send()
            for chunk in range(chunks):
                to_right(chunk).wait_send()
                mixed_right(chunk).wait_send()

        @pl.when(has_left)
        def _():
            fields_left.wait_send()
            for chunk in range(chunks):
                to_left(chunk).wait_send()
                mixed_left(chunk).wait_send()

        for turn in range(3):
            wait_bytes(gathered.at[turn], rs_send.at[turn])
            wait_bytes(others(turn), ag_send.at[turn])
        for turn in range(2):

            @pl.when(has_right)
            def _():
                wait_bytes(full.at[turn, :, low_rows, :], low_send.at[turn])

            @pl.when(has_left)
            def _():
                wait_bytes(full.at[turn, :, high_rows, :], high_send.at[turn])

            wait_bytes(group_note.at[turn, pl.ds(0, groups - 1)], note_send.at[turn])
            wait_bytes(block_note.at[turn, pl.ds(0, blocks - 1)], sum_send.at[turn])

    bf16 = jnp.bfloat16
    dma = pltpu.SemaphoreType.DMA
    scratch = [
        pltpu.SMEM((TAPS,), F32),
        pltpu.SMEM((2, TAPS), jnp.int32),
        pltpu.VMEM((obs_rows, LANES), jnp.int32),
        pltpu.VMEM((obs_rows, LANES), jnp.int32),
        pltpu.VMEM((obs_rows, LANES), jnp.int32),
        pltpu.VMEM((obs_rows, LANES), F32),
        pltpu.VMEM((obs_rows, LANES), F32),
        pltpu.VMEM((levels, members, width, depth), bf16),
        pltpu.VMEM((levels, members, HALO, depth), bf16),
        pltpu.VMEM((levels, members, HALO, depth), bf16),
        pltpu.VMEM((levels, members, HALO, depth), bf16),
        pltpu.VMEM((levels, members, HALO, depth), bf16),
        pltpu.VMEM((2, members, halves, HALO, LANES), F32),
        pltpu.VMEM((2, members, halves, HALO, LANES), F32),
        pltpu.VMEM((2, planes, rows, LANES), F32),
        pltpu.VMEM((planes, rows, LANES), F32),
        pltpu.VMEM((members, halves, rows, LANES), F32),
        pltpu.VMEM((3, members, halves, rows, LANES), F32),
        pltpu.VMEM((members, halves, width, LANES), F32),
        pltpu.VMEM((3, planes, width, LANES), F32),
        pltpu.VMEM((3, groups - 1, width, LANES), F32),
        pltpu.VMEM((3, planes, rows, LANES), F32),
        pltpu.VMEM((2, 1, LANES), F32),
        pltpu.VMEM((2, groups, 1, LANES), F32),
        pltpu.VMEM((2, 1, LANES), F32),
        pltpu.VMEM((2, blocks, 1, LANES), F32),
        pltpu.SemaphoreType.REGULAR((5, 2)),
        dma((10,)),
        dma((2, chunks)), dma((2, chunks)), dma((2, chunks)), dma((2, chunks)), dma((2,)), dma((2,)),
        dma((3,)), dma((3,)), dma((3,)), dma((3,)),
        dma((2,)), dma((2,)), dma((2,)), dma((2,)),
        dma((2,)), dma((2,)), dma((2,)), dma((2,)),
    ]
    return kernel, scratch


def solution(mesh):
    groups, blocks = mesh.shape["mem"], mesh.shape["col"]

    def per_device(perturbations, loc_weights, offsets, obs_x, obs_y, obs_t, innovations, obs_rinv):
        levels, members, width, depth = perturbations.shape
        obs_rows = obs_x.shape[0] // LANES
        kernel, scratch = make_kernel(groups, blocks, levels, members, width, depth, obs_rows)
        vmem = pl.BlockSpec(memory_space=pltpu.VMEM)
        hbm = pl.BlockSpec(memory_space=pl.ANY)
        return pl.pallas_call(
            kernel,
            out_shape=(
                pltpu.VMEM((members, width, depth), F32),
                pltpu.VMEM((levels, width, depth), F32),
            ),
            in_specs=[hbm] * 8,
            out_specs=(vmem,) * 2,
            scratch_shapes=scratch,
            compiler_params=pltpu.CompilerParams(collective_id=0, has_side_effects=True),
        )(
            perturbations, loc_weights, offsets.T,
            *(v.reshape(obs_rows, LANES) for v in (obs_x, obs_y, obs_t, innovations, obs_rinv)),
        )

    return jax.shard_map(
        per_device,
        mesh=mesh,
        in_specs=(P(None, "mem", "col", None), P(), P()) + (P("col"),) * 5,
        out_specs=(P("mem", "col", None), P(None, "col", None)),
        check_vma=False,
    )
```

```python
import jax
import jax.numpy as jnp
from jax import lax
from jax.experimental import pallas as pl
from jax.experimental.pallas import tpu as pltpu
from jax.sharding import PartitionSpec as P

TAPS = 7
RADIUS = 4
LANES = 128
HALO = 2 * RADIUS
F32 = jnp.float32
UNROLL = 4
OBS_UNROLL = 4
CHUNK = 8
MESH = pl.DeviceIdType.MESH


def make_kernel(groups, blocks, levels, members, width, depth, obs_rows):
    halves = depth // LANES
    planes = levels * halves
    rows = width + 2 * HALO
    chunks = members // CHUNK
    own = pl.ds(HALO, width)
    low_rows = pl.ds(0, HALO)
    high_rows = pl.ds(HALO + width, HALO)
    last_own = pl.ds(width, HALO)
    first_own = pl.ds(HALO, HALO)

    def kernel(
        pert, weights_in, offsets_in, obs_x_in, obs_y_in, obs_t_in, innov_in, rinv_in,
        control, increment,
        weights, offsets, obs_x, obs_y, obs_t, innov, rinv,
        p, p_low, p_high, p_right, p_left, mix_out, mix_in, fields, z, mixed, resid, second, part, gathered, full,
        note, group_note, sums, block_note,
        hello, load_sem, mixed_send, mixed_recv, halo_send, halo_recv, field_send, field_recv,
        rs_send, rs_recv, ag_send, ag_recv, low_send, low_recv, high_send, high_recv,
        note_send, note_recv, sum_send, sum_recv,
    ):
        me = lax.axis_index("mem")
        col = lax.axis_index("col")
        right, left = col + 1, col - 1
        has_left, has_right = col > 0, col < blocks - 1

        barrier = pltpu.get_barrier_semaphore()

        def greet(target):
            pl.semaphore_signal(barrier, inc=1, device_id=target, device_id_type=MESH)

        for step in range(1, groups):
            greet((lax.rem(me + step, groups), col))

        @pl.when(has_right)
        def _():
            greet((me, right))

        @pl.when(has_left)
        def _():
            greet((me, left))

        loads = [
            pltpu.make_async_copy(source, target, load_sem.at[at])
            for at, (source, target) in enumerate(
                (
                    (obs_x_in, obs_x), (obs_y_in, obs_y), (obs_t_in, obs_t), (innov_in, innov),
                    (rinv_in, rinv), (weights_in, weights), (offsets_in, offsets), (pert, p),
                    (pert.at[:, :, pl.ds(width - HALO, HALO), :], p_right),
                    (pert.at[:, :, pl.ds(0, HALO), :], p_left),
                )
            )
        ]
        for copy in loads:
            copy.start()
        edge_loads, load, loads = loads[-2:], loads[-3], loads[:-3]
        def hello_sides(turn):
            away = 1 << turn
            return (0, col + away, col + away < blocks), (1, col - away, col >= away)

        def say_hello(turn):
            for side, peer, there in hello_sides(turn):

                @pl.when(there)
                def _():
                    pl.semaphore_signal(
                        hello.at[turn, side], inc=1, device_id=(me, peer), device_id_type=MESH
                    )

        def hear_hello(turn):
            for side, _, there in hello_sides(turn):

                @pl.when(there)
                def _():
                    pl.semaphore_wait(hello.at[turn, 1 - side], 1)

        lanes8 = lax.broadcasted_iota(jnp.int32, (1, LANES), 1)
        cell_rows = lax.broadcasted_iota(jnp.int32, (levels * width, LANES), 0)
        depth_rows = lax.broadcasted_iota(jnp.int32, (depth, LANES), 0)

        def place(chunk, total):
            left_side, right_side = [], []
            for more in range(OBS_UNROLL):
                at = pl.ds(chunk * OBS_UNROLL + more, 1)
                cell = obs_t[at, :] * width + (obs_x[at, :] - col * width)
                r = rinv[at, :]
                hit = cell_rows == cell
                pieces = []
                for value in (r * innov[at, :], r):
                    rest = value
                    for _ in range(3):
                        piece = rest.astype(jnp.bfloat16)
                        rest = rest - piece.astype(F32)
                        pieces.append(jnp.where(hit, piece.astype(F32), 0.0).astype(jnp.bfloat16))
                left_side.append(jnp.concatenate(pieces, axis=0))
                right_side.append(
                    jnp.where(depth_rows == obs_y[at, :], 1.0, 0.0).astype(jnp.bfloat16)
                )
            return total + lax.dot_general(
                jnp.concatenate(left_side, axis=1),
                jnp.concatenate(right_side, axis=1),
                (((1,), (1,)), ((), ())),
                preferred_element_type=F32,
            )

        for copy in loads:
            copy.wait()
        spread = lax.fori_loop(
            0, obs_rows // OBS_UNROLL, place, jnp.zeros((6 * levels * width, depth), F32)
        )
        cells = levels * width
        for which in range(2):
            base = 3 * which * cells
            summed = (
                spread[base : base + cells]
                + spread[base + cells : base + 2 * cells]
                + spread[base + 2 * cells : base + 3 * cells]
            )
            for level in range(levels):
                for half in range(halves):
                    fields[which, level * halves + half, own, :] = summed[
                        level * width : (level + 1) * width, half * LANES : (half + 1) * LANES
                    ]

        def remote(source, target, send, recv, device):
            return pltpu.make_async_remote_copy(
                src_ref=source, dst_ref=target, send_sem=send, recv_sem=recv,
                device_id=device, device_id_type=MESH,
            )

        def members_of(chunk):
            return pl.ds(chunk * CHUNK, CHUNK)

        def to_right(chunk):
            return remote(
                p_right.at[:, members_of(chunk)], p_low.at[:, members_of(chunk)],
                halo_send.at[0, chunk], halo_recv.at[0, chunk], (me, right),
            )

        def to_left(chunk):
            return remote(
                p_left.at[:, members_of(chunk)], p_high.at[:, members_of(chunk)],
                halo_send.at[1, chunk], halo_recv.at[1, chunk], (me, left),
            )

        def mixed_right(chunk):
            return remote(
                mix_out.at[0, members_of(chunk)], mix_in.at[0, members_of(chunk)],
                mixed_send.at[0, chunk], mixed_recv.at[0, chunk], (me, right),
            )

        def mixed_left(chunk):
            return remote(
                mix_out.at[1, members_of(chunk)], mix_in.at[1, members_of(chunk)],
                mixed_send.at[1, chunk], mixed_recv.at[1, chunk], (me, left),
            )

        def send_halo(*which):
            @pl.when(has_right)
            def _():
                for chunk in which:
                    to_right(chunk).start()

            @pl.when(has_left)
            def _():
                for chunk in which:
                    to_left(chunk).start()

        fields_right = remote(
            fields.at[:, :, last_own, :], fields.at[:, :, low_rows, :],
            field_send.at[0], field_recv.at[0], (me, right),
        )
        fields_left = remote(
            fields.at[:, :, first_own, :], fields.at[:, :, high_rows, :],
            field_send.at[1], field_recv.at[1], (me, left),
        )
        tap_weight = [weights[s] for s in range(TAPS)]
        along = [offsets[0, s] for s in range(TAPS)]
        across = [offsets[1, s] for s in range(TAPS)]

        def mix(source, at, k, out=False):
            for half in range(halves):
                total = None
                for level in range(levels):
                    term = source[level, k, :, half * LANES : (half + 1) * LANES].astype(F32) * z[
                        level * halves + half, at, :
                    ]
                    total = term if total is None else total + term
                mixed[k, half, at, :] = total
                if out:
                    mix_out[0, k, half] = total[width - HALO :]
                    mix_out[1, k, half] = total[:HALO]

        def mix_own(out=False):
            def step(k, carry):
                for more in range(UNROLL):
                    mix(p, own, UNROLL * k + more, out)
                return carry

            lax.fori_loop(0, members // UNROLL, step, 0)

        reach = width + 2 * RADIUS
        row_at = lax.broadcasted_iota(jnp.int32, (reach, LANES), 0) + (col * width - RADIUS)
        keep = jnp.where((row_at >= 0) & (row_at < blocks * width), 1.0, 0.0)

        def turns(amounts):
            spots = [lax.broadcasted_iota(jnp.int32, (1, LANES), 1) - v for v in amounts]
            return (
                [jnp.where(v < 0, v + LANES, v) for v in amounts],
                [(s >= 0) & (s < LANES) for s in spots],
            )

        back, forth = turns(across), turns([-v for v in across])

        def stencil(source, starts, count, moves):
            total = [None] * halves
            for s in range(TAPS):
                turned = [
                    pltpu.roll(source(half, pl.ds(starts[s], count)), moves[0][s], 1)
                    for half in range(halves)
                ]
                for half in range(halves):
                    term = tap_weight[s] * jnp.where(
                        moves[1][s], turned[half], turned[1 - half]
                    )
                    total[half] = term if total[half] is None else total[half] + term
            return total

        back_starts = [RADIUS - v for v in along]
        forth_starts = [HALO + v for v in along]

        def first_edges(chunk):
            pl.when(has_left)(lambda: mixed_right(chunk).wait_recv())
            pl.when(has_right)(lambda: mixed_left(chunk).wait_recv())
            for more in range(CHUNK):
                k = CHUNK * chunk + more
                for half in range(halves):
                    mixed[k, half, low_rows, :] = mix_in[0, k, half]
                    mixed[k, half, high_rows, :] = mix_in[1, k, half]

        def later_edges(chunk):
            for more in range(CHUNK):
                mix(p_low, low_rows, CHUNK * chunk + more)
                mix(p_high, high_rows, CHUNK * chunk + more)

        def arriving_edges(chunk):
            pl.when(has_left)(lambda: to_right(chunk).wait_recv())
            pl.when(has_right)(lambda: to_left(chunk).wait_recv())
            later_edges(chunk)

        def apply(turn, edges):
            def step(chunk, so_far):
                edges(chunk)
                for more in range(CHUNK):
                    k = CHUNK * chunk + more
                    total = stencil(lambda h, rows_at: mixed[k, h, rows_at, :], back_starts, reach, back)
                    for half in range(halves):
                        resid[turn, k, half, pl.ds(RADIUS, reach), :] = total[half] * keep
                for more in range(CHUNK):
                    k = CHUNK * chunk + more
                    total = stencil(
                        lambda h, rows_at: resid[turn, k, h, rows_at, :], forth_starts, width, forth
                    )
                    so_far = tuple(
                        so_far[level * halves + half]
                        + p[level, k, :, half * LANES : (half + 1) * LANES].astype(F32) * total[half]
                        for level in range(levels)
                        for half in range(halves)
                    )
                return so_far

            summed = lax.fori_loop(
                0, chunks, step, tuple(jnp.zeros((width, LANES), F32) for _ in range(planes))
            )
            for plane in range(planes):
                part[turn, plane] = summed[plane]

        def wait_bytes(ref, sem):
            pltpu.make_async_copy(ref, ref, sem).wait()

        def start_sums(turn):
            for step in range(1, groups):
                peer = lax.rem(me + step, groups)
                remote(
                    part.at[turn, peer], gathered.at[turn, step - 1],
                    rs_send.at[turn], rs_recv.at[turn], (peer, col),
                ).start()

        def finish_sums(turn):
            wait_bytes(gathered.at[turn], rs_recv.at[turn])
            total = part[turn, me]
            for s in range(groups - 1):
                total = total + gathered[turn, s]
            full[turn, me, own, :] = total
            return total

        def start_edges(turn):
            @pl.when(has_right)
            def _():
                for step in range(groups):
                    remote(
                        full.at[turn, me, last_own, :], full.at[turn, me, low_rows, :],
                        low_send.at[turn], low_recv.at[turn], (lax.rem(me + step, groups), right),
                    ).start()

            @pl.when(has_left)
            def _():
                for step in range(groups):
                    remote(
                        full.at[turn, me, first_own, :], full.at[turn, me, high_rows, :],
                        high_send.at[turn], high_recv.at[turn], (lax.rem(me + step, groups), left),
                    ).start()

        def start_group(turn):
            spot = full.at[turn, me, own, :]
            for step in range(1, groups):
                remote(
                    spot, spot, ag_send.at[turn], ag_recv.at[turn], (lax.rem(me + step, groups), col)
                ).start()

        def others(turn):
            return full.at[turn, pl.ds(0, groups - 1), own, :]

        def finish_own(turn):
            wait_bytes(others(turn), ag_recv.at[turn])

        def finish_edges(turn):
            @pl.when(has_left)
            def _():
                wait_bytes(full.at[turn, :, low_rows, :], low_recv.at[turn])

            @pl.when(has_right)
            def _():
                wait_bytes(full.at[turn, :, high_rows, :], high_recv.at[turn])

        def send_note(which, values):
            row = jnp.zeros((1, LANES), F32)
            for at, value in enumerate(values):
                row = jnp.where(lanes8 == at, value, row)
            note[which] = row
            group_note[which, me] = row
            for step in range(1, groups):
                remote(
                    note.at[which], group_note.at[which, me],
                    note_send.at[which], note_recv.at[which], (lax.rem(me + step, groups), col),
                ).start()

        def pass_note(which):
            wait_bytes(group_note.at[which, pl.ds(0, groups - 1)], note_recv.at[which])
            total = group_note[which, 0]
            for other in range(1, groups):
                total = total + group_note[which, other]
            sums[which] = total
            block_note[which, col] = total
            for step in range(1, blocks):
                remote(
                    sums.at[which], block_note.at[which, col],
                    sum_send.at[which], sum_recv.at[which], (me, lax.rem(col + step, blocks)),
                ).start()

        def read_note(which, count):
            wait_bytes(block_note.at[which, pl.ds(0, blocks - 1)], sum_recv.at[which])
            total = block_note[which, 0]
            for other in range(1, blocks):
                total = total + block_note[which, other]
            return [
                jnp.sum(jnp.where(lanes8 == at, total, 0.0), axis=1, keepdims=True)
                for at in range(count)
            ]

        def all_of(value):
            return jnp.sum(jnp.sum(value, axis=0, keepdims=True), axis=1, keepdims=True)

        load.wait()
        for plane in range(planes):
            z[plane, own, :] = fields[0, plane, own, :]
        mix_own(True)
        beside = lax.div(col + blocks - 1, blocks) + lax.div(2 * blocks - 2 - col, blocks)
        pl.semaphore_wait(barrier, groups - 1 + beside)

        @pl.when(has_right)
        def _():
            for chunk in range(chunks):
                mixed_right(chunk).start()
            fields_right.start()

        @pl.when(has_left)
        def _():
            for chunk in range(chunks):
                mixed_left(chunk).start()
            fields_left.start()

        for copy in edge_loads:
            copy.wait()
        send_halo(0)
        say_hello(0)

        @pl.when(col == 0)
        def _():
            p_low[...] = jnp.zeros(p_low.shape, p_low.dtype)
            mix_in[0] = jnp.zeros((members, halves, HALO, LANES), F32)
            fields[:, :, low_rows, :] = jnp.zeros((2, planes, HALO, LANES), F32)
            full[:, :, low_rows, :] = jnp.zeros((3, planes, HALO, LANES), F32)

        @pl.when(col == blocks - 1)
        def _():
            p_high[...] = jnp.zeros(p_high.shape, p_high.dtype)
            mix_in[1] = jnp.zeros((members, halves, HALO, LANES), F32)
            fields[:, :, high_rows, :] = jnp.zeros((2, planes, HALO, LANES), F32)
            full[:, :, high_rows, :] = jnp.zeros((3, planes, HALO, LANES), F32)

        hear_hello(0)
        say_hello(1)

        hear_hello(1)
        say_hello(2)
        apply(0, first_edges)
        hear_hello(2)
        say_hello(3)
        start_sums(0)
        send_halo(1, 2)

        def square(k, total):
            for half in range(halves):
                value = resid[0, k, half, own, :]
                total = total + value * value
            return total

        norm = all_of(lax.fori_loop(0, members, square, jnp.zeros((width, LANES), F32)))
        mine = finish_sums(0)
        hear_hello(3)
        say_hello(4)
        start_edges(0)
        start_group(0)
        send_halo(3)
        send_note(0, [norm, all_of(fields[1, me, own, :] * mine * mine)])
        finish_own(0)

        def image_of_first(at):
            for plane in range(planes):
                z[plane, at, :] = (
                    fields[0, plane, at, :] + fields[1, plane, at, :] * full[0, plane, at, :]
                )


        image_of_first(own)
        mix_own()
        hear_hello(4)
        pass_note(0)
        finish_edges(0)

        @pl.when(has_left)
        def _():
            fields_right.wait_recv()

        @pl.when(has_right)
        def _():
            fields_left.wait_recv()

        image_of_first(low_rows)
        image_of_first(high_rows)
        apply(1, arriving_edges)
        start_sums(1)
        finish_sums(1)
        start_edges(1)
        start_group(1)
        norm_0, bend_0 = read_note(0, 2)
        curve_0 = norm_0 + bend_0
        step_0 = norm_0 / curve_0
        finish_own(1)

        def image_of_second(at):
            for plane in range(planes):
                z[plane, at, :] = (fields[0, plane, at, :] - step_0 * z[plane, at, :]) + fields[
                    1, plane, at, :
                ] * (full[0, plane, at, :] - step_0 * full[1, plane, at, :])

        image_of_second(own)
        mix_own()
        finish_edges(1)
        image_of_second(low_rows)
        image_of_second(high_rows)
        apply(2, later_edges)
        start_sums(2)

        def products(k, so_far):
            ab, ac, bb, bc, cc = so_far
            for half in range(halves):
                a = resid[0, k, half, own, :]
                b = a - step_0 * resid[1, k, half, own, :]
                c = resid[2, k, half, own, :]
                second[k, half] = b
                ab, ac, bb, bc, cc = ab + a * b, ac + a * c, bb + b * b, bc + b * c, cc + c * c
            return ab, ac, bb, bc, cc

        inner = [
            all_of(v)
            for v in lax.fori_loop(
                0, members, products, tuple(jnp.zeros((width, LANES), F32) for _ in range(5))
            )
        ]
        mine_c = finish_sums(2)
        mine_a = full[0, me, own, :]
        mine_b = mine_a - step_0 * full[1, me, own, :]
        weight = fields[1, me, own, :]
        wb, wc = weight * mine_b, weight * mine_c
        bends = [all_of(v) for v in (wb * mine_a, wc * mine_a, wb * mine_b, wc * mine_b, wc * mine_c)]
        send_note(1, inner + bends)
        start_group(2)
        pass_note(1)
        g_ab, g_ac, g_bb, g_bc, g_cc, e_ab, e_ac, e_bb, e_bc, e_cc = read_note(1, 10)
        finish_own(2)

        def form(aa, ab, ac, bb, bc, cc, u):
            a, b, c = u
            return (
                a * a * aa + b * b * bb + c * c * cc + 2.0 * (a * b * ab + a * c * ac + b * c * bc)
            )

        h = (curve_0, g_ab + e_ab, g_ac + e_ac, g_bb + e_bb, g_bc + e_bc, g_cc + e_cc)
        one = jnp.ones_like(norm_0)
        ratio_0 = g_bb / norm_0
        d1 = (ratio_0, one, 0.0 * one)
        step_1 = g_bb / form(*h, d1)
        mixing = step_1 * ratio_0 / step_0
        r2 = (-mixing, one + mixing, -step_1)
        norm_2 = form(norm_0, g_ab, g_ac, g_bb, g_bc, g_cc, r2)
        ratio_1 = norm_2 / g_bb
        d2 = tuple(r + ratio_1 * d for r, d in zip(r2, d1))
        step_2 = norm_2 / form(*h, d2)
        in_a = step_0 + step_1 * d1[0] + step_2 * d2[0]
        in_b = step_1 * d1[1] + step_2 * d2[1]
        in_c = step_1 * d1[2] + step_2 * d2[2]

        def write(step, carry):
            for more in range(UNROLL):
                k = UNROLL * step + more
                for half in range(halves):
                    control[k, :, half * LANES : (half + 1) * LANES] = (
                        in_a * resid[0, k, half, own, :]
                        + in_b * second[k, half]
                        + in_c * resid[2, k, half, own, :]
                    )
            return carry

        lax.fori_loop(0, members // UNROLL, write, 0)
        for level in range(levels):
            for half in range(halves):
                plane = level * halves + half
                a = full[0, plane, own, :]
                b = a - step_0 * full[1, plane, own, :]
                increment[level, :, half * LANES : (half + 1) * LANES] = (
                    in_a * a + in_b * b + in_c * full[2, plane, own, :]
                )

        @pl.when(has_right)
        def _():
            fields_right.wait_send()
            for chunk in range(chunks):
                to_right(chunk).wait_send()
                mixed_right(chunk).wait_send()

        @pl.when(has_left)
        def _():
            fields_left.wait_send()
            for chunk in range(chunks):
                to_left(chunk).wait_send()
                mixed_left(chunk).wait_send()

        for turn in range(3):
            wait_bytes(gathered.at[turn], rs_send.at[turn])
            wait_bytes(others(turn), ag_send.at[turn])
        for turn in range(2):

            @pl.when(has_right)
            def _():
                wait_bytes(full.at[turn, :, low_rows, :], low_send.at[turn])

            @pl.when(has_left)
            def _():
                wait_bytes(full.at[turn, :, high_rows, :], high_send.at[turn])

            wait_bytes(group_note.at[turn, pl.ds(0, groups - 1)], note_send.at[turn])
            wait_bytes(block_note.at[turn, pl.ds(0, blocks - 1)], sum_send.at[turn])

    bf16 = jnp.bfloat16
    dma = pltpu.SemaphoreType.DMA
    scratch = [
        pltpu.SMEM((TAPS,), F32),
        pltpu.SMEM((2, TAPS), jnp.int32),
        pltpu.VMEM((obs_rows, LANES), jnp.int32),
        pltpu.VMEM((obs_rows, LANES), jnp.int32),
        pltpu.VMEM((obs_rows, LANES), jnp.int32),
        pltpu.VMEM((obs_rows, LANES), F32),
        pltpu.VMEM((obs_rows, LANES), F32),
        pltpu.VMEM((levels, members, width, depth), bf16),
        pltpu.VMEM((levels, members, HALO, depth), bf16),
        pltpu.VMEM((levels, members, HALO, depth), bf16),
        pltpu.VMEM((levels, members, HALO, depth), bf16),
        pltpu.VMEM((levels, members, HALO, depth), bf16),
        pltpu.VMEM((2, members, halves, HALO, LANES), F32),
        pltpu.VMEM((2, members, halves, HALO, LANES), F32),
        pltpu.VMEM((2, planes, rows, LANES), F32),
        pltpu.VMEM((planes, rows, LANES), F32),
        pltpu.VMEM((members, halves, rows, LANES), F32),
        pltpu.VMEM((3, members, halves, rows, LANES), F32),
        pltpu.VMEM((members, halves, width, LANES), F32),
        pltpu.VMEM((3, planes, width, LANES), F32),
        pltpu.VMEM((3, groups - 1, width, LANES), F32),
        pltpu.VMEM((3, planes, rows, LANES), F32),
        pltpu.VMEM((2, 1, LANES), F32),
        pltpu.VMEM((2, groups, 1, LANES), F32),
        pltpu.VMEM((2, 1, LANES), F32),
        pltpu.VMEM((2, blocks, 1, LANES), F32),
        pltpu.SemaphoreType.REGULAR((5, 2)),
        dma((10,)),
        dma((2, chunks)), dma((2, chunks)), dma((2, chunks)), dma((2, chunks)), dma((2,)), dma((2,)),
        dma((3,)), dma((3,)), dma((3,)), dma((3,)),
        dma((2,)), dma((2,)), dma((2,)), dma((2,)),
        dma((2,)), dma((2,)), dma((2,)), dma((2,)),
    ]
    return kernel, scratch


def solution(mesh):
    groups, blocks = mesh.shape["mem"], mesh.shape["col"]

    def per_device(perturbations, loc_weights, offsets, obs_x, obs_y, obs_t, innovations, obs_rinv):
        levels, members, width, depth = perturbations.shape
        obs_rows = obs_x.shape[0] // LANES
        kernel, scratch = make_kernel(groups, blocks, levels, members, width, depth, obs_rows)
        vmem = pl.BlockSpec(memory_space=pltpu.VMEM)
        hbm = pl.BlockSpec(memory_space=pl.ANY)
        kept = pl.pallas_call(
            kernel,
            out_shape=(
                pltpu.VMEM((members, width, depth), F32),
                pltpu.VMEM((levels, width, depth), F32),
            ),
            in_specs=[hbm] * 8,
            out_specs=(vmem,) * 2,
            scratch_shapes=scratch,
            compiler_params=pltpu.CompilerParams(collective_id=0, has_side_effects=True),
        )(
            perturbations, loc_weights, offsets.T,
            *(v.reshape(obs_rows, LANES) for v in (obs_x, obs_y, obs_t, innovations, obs_rinv)),
        )

        def put_out(control, increment, control_out, increment_out, sem):
            copies = [
                pltpu.make_async_copy(control, control_out, sem.at[0]),
                pltpu.make_async_copy(increment, increment_out, sem.at[1]),
            ]
            for copy in copies:
                copy.start()
            for copy in copies:
                copy.wait()

        return pl.pallas_call(
            put_out,
            out_shape=(
                jax.ShapeDtypeStruct((members, width, depth), F32),
                jax.ShapeDtypeStruct((levels, width, depth), F32),
            ),
            in_specs=[vmem] * 2,
            out_specs=(pl.BlockSpec(memory_space=pltpu.HBM),) * 2,
            scratch_shapes=[pltpu.SemaphoreType.DMA((2,))],
        )(*(pltpu.with_memory_space_constraint(v, pltpu.VMEM) for v in kept))

    return jax.shard_map(
        per_device,
        mesh=mesh,
        in_specs=(P(None, "mem", "col", None), P(), P()) + (P("col"),) * 5,
        out_specs=(P("mem", "col", None), P(None, "col", None)),
        check_vma=False,
    )
```

```python
import jax
import jax.numpy as jnp
from jax import lax
from jax.experimental import pallas as pl
from jax.experimental.pallas import tpu as pltpu
from jax.sharding import PartitionSpec as P

TAPS = 7
RADIUS = 4
LANES = 128
HALO = 2 * RADIUS
F32 = jnp.float32
UNROLL = 4
OBS_UNROLL = 4
CHUNK = 8
MESH = pl.DeviceIdType.MESH


def make_kernel(groups, blocks, levels, members, width, depth, obs_rows):
    halves = depth // LANES
    planes = levels * halves
    rows = width + 2 * HALO
    chunks = members // CHUNK
    own = pl.ds(HALO, width)
    low_rows = pl.ds(0, HALO)
    high_rows = pl.ds(HALO + width, HALO)
    last_own = pl.ds(width, HALO)
    first_own = pl.ds(HALO, HALO)

    def kernel(
        pert, weights_in, offsets_in, obs_x_in, obs_y_in, obs_t_in, innov_in, rinv_in,
        control, increment,
        weights, offsets, obs_x, obs_y, obs_t, innov, rinv,
        p, p_low, p_high, p_right, p_left, mix_out, mix_in, fields, z, mixed, resid, second, part, gathered, full,
        note, group_note, sums, block_note,
        hello, load_sem, mixed_send, mixed_recv, halo_send, halo_recv, field_send, field_recv,
        rs_send, rs_recv, ag_send, ag_recv, low_send, low_recv, high_send, high_recv,
        note_send, note_recv, sum_send, sum_recv,
    ):
        me = lax.axis_index("mem")
        col = lax.axis_index("col")
        right, left = col + 1, col - 1
        has_left, has_right = col > 0, col < blocks - 1

        barrier = pltpu.get_barrier_semaphore()

        def greet(target):
            pl.semaphore_signal(barrier, inc=1, device_id=target, device_id_type=MESH)

        for step in range(1, groups):
            greet((lax.rem(me + step, groups), col))

        @pl.when(has_right)
        def _():
            greet((me, right))

        @pl.when(has_left)
        def _():
            greet((me, left))

        loads = [
            pltpu.make_async_copy(source, target, load_sem.at[at])
            for at, (source, target) in enumerate(
                (
                    (obs_x_in, obs_x), (obs_y_in, obs_y), (obs_t_in, obs_t), (innov_in, innov),
                    (rinv_in, rinv), (weights_in, weights), (offsets_in, offsets), (pert, p),
                    (pert.at[:, :, pl.ds(width - HALO, HALO), :], p_right),
                    (pert.at[:, :, pl.ds(0, HALO), :], p_left),
                )
            )
        ]
        for copy in loads:
            copy.start()
        edge_loads, load, loads = loads[-2:], loads[-3], loads[:-3]
        def hello_sides(turn):
            away = 1 << turn
            return (0, col + away, col + away < blocks), (1, col - away, col >= away)

        def say_hello(turn):
            for side, peer, there in hello_sides(turn):

                @pl.when(there)
                def _():
                    pl.semaphore_signal(
                        hello.at[turn, side], inc=1, device_id=(me, peer), device_id_type=MESH
                    )

        def hear_hello(turn):
            for side, _, there in hello_sides(turn):

                @pl.when(there)
                def _():
                    pl.semaphore_wait(hello.at[turn, 1 - side], 1)

        lanes8 = lax.broadcasted_iota(jnp.int32, (1, LANES), 1)
        cell_rows = lax.broadcasted_iota(jnp.int32, (levels * width, LANES), 0)
        depth_rows = lax.broadcasted_iota(jnp.int32, (depth, LANES), 0)

        def place(chunk, total):
            left_side, right_side = [], []
            for more in range(OBS_UNROLL):
                at = pl.ds(chunk * OBS_UNROLL + more, 1)
                cell = obs_t[at, :] * width + (obs_x[at, :] - col * width)
                r = rinv[at, :]
                hit = cell_rows == cell
                pieces = []
                for value in (r * innov[at, :], r):
                    rest = value
                    for _ in range(3):
                        piece = rest.astype(jnp.bfloat16)
                        rest = rest - piece.astype(F32)
                        pieces.append(jnp.where(hit, piece.astype(F32), 0.0).astype(jnp.bfloat16))
                left_side.append(jnp.concatenate(pieces, axis=0))
                right_side.append(
                    jnp.where(depth_rows == obs_y[at, :], 1.0, 0.0).astype(jnp.bfloat16)
                )
            return total + lax.dot_general(
                jnp.concatenate(left_side, axis=1),
                jnp.concatenate(right_side, axis=1),
                (((1,), (1,)), ((), ())),
                preferred_element_type=F32,
            )

        for copy in loads:
            copy.wait()
        spread = lax.fori_loop(
            0, obs_rows // OBS_UNROLL, place, jnp.zeros((6 * levels * width, depth), F32)
        )
        cells = levels * width
        for which in range(2):
            base = 3 * which * cells
            summed = (
                spread[base : base + cells]
                + spread[base + cells : base + 2 * cells]
                + spread[base + 2 * cells : base + 3 * cells]
            )
            for level in range(levels):
                for half in range(halves):
                    fields[which, level * halves + half, own, :] = summed[
                        level * width : (level + 1) * width, half * LANES : (half + 1) * LANES
                    ]

        def remote(source, target, send, recv, device):
            return pltpu.make_async_remote_copy(
                src_ref=source, dst_ref=target, send_sem=send, recv_sem=recv,
                device_id=device, device_id_type=MESH,
            )

        def members_of(chunk):
            return pl.ds(chunk * CHUNK, CHUNK)

        def to_right(chunk):
            return remote(
                p_right.at[:, members_of(chunk)], p_low.at[:, members_of(chunk)],
                halo_send.at[0, chunk], halo_recv.at[0, chunk], (me, right),
            )

        def to_left(chunk):
            return remote(
                p_left.at[:, members_of(chunk)], p_high.at[:, members_of(chunk)],
                halo_send.at[1, chunk], halo_recv.at[1, chunk], (me, left),
            )

        def mixed_right(chunk):
            return remote(
                mix_out.at[0, members_of(chunk)], mix_in.at[0, members_of(chunk)],
                mixed_send.at[0, chunk], mixed_recv.at[0, chunk], (me, right),
            )

        def mixed_left(chunk):
            return remote(
                mix_out.at[1, members_of(chunk)], mix_in.at[1, members_of(chunk)],
                mixed_send.at[1, chunk], mixed_recv.at[1, chunk], (me, left),
            )

        def send_halo(*which):
            @pl.when(has_right)
            def _():
                for chunk in which:
                    to_right(chunk).start()

            @pl.when(has_left)
            def _():
                for chunk in which:
                    to_left(chunk).start()

        fields_right = remote(
            fields.at[:, :, last_own, :], fields.at[:, :, low_rows, :],
            field_send.at[0], field_recv.at[0], (me, right),
        )
        fields_left = remote(
            fields.at[:, :, first_own, :], fields.at[:, :, high_rows, :],
            field_send.at[1], field_recv.at[1], (me, left),
        )
        tap_weight = [weights[s] for s in range(TAPS)]
        along = [offsets[0, s] for s in range(TAPS)]
        across = [offsets[1, s] for s in range(TAPS)]

        def mix(source, at, k, out=False):
            for half in range(halves):
                total = None
                for level in range(levels):
                    term = source[level, k, :, half * LANES : (half + 1) * LANES].astype(F32) * z[
                        level * halves + half, at, :
                    ]
                    total = term if total is None else total + term
                mixed[k, half, at, :] = total
                if out:
                    mix_out[0, k, half] = total[width - HALO :]
                    mix_out[1, k, half] = total[:HALO]

        def mix_own(out=False):
            def step(k, carry):
                for more in range(UNROLL):
                    mix(p, own, UNROLL * k + more, out)
                return carry

            lax.fori_loop(0, members // UNROLL, step, 0)

        reach = width + 2 * RADIUS
        row_at = lax.broadcasted_iota(jnp.int32, (reach, LANES), 0) + (col * width - RADIUS)
        keep = jnp.where((row_at >= 0) & (row_at < blocks * width), 1.0, 0.0)

        def turns(amounts):
            spots = [lax.broadcasted_iota(jnp.int32, (1, LANES), 1) - v for v in amounts]
            return (
                [jnp.where(v < 0, v + LANES, v) for v in amounts],
                [(s >= 0) & (s < LANES) for s in spots],
            )

        back, forth = turns(across), turns([-v for v in across])

        def stencil(source, starts, count, moves):
            total = [None] * halves
            for s in range(TAPS):
                turned = [
                    pltpu.roll(source(half, pl.ds(starts[s], count)), moves[0][s], 1)
                    for half in range(halves)
                ]
                for half in range(halves):
                    term = tap_weight[s] * jnp.where(
                        moves[1][s], turned[half], turned[1 - half]
                    )
                    total[half] = term if total[half] is None else total[half] + term
            return total

        back_starts = [RADIUS - v for v in along]
        forth_starts = [HALO + v for v in along]

        def first_edges(chunk):
            pl.when(has_left)(lambda: mixed_right(chunk).wait_recv())
            pl.when(has_right)(lambda: mixed_left(chunk).wait_recv())
            for more in range(CHUNK):
                k = CHUNK * chunk + more
                for half in range(halves):
                    mixed[k, half, low_rows, :] = mix_in[0, k, half]
                    mixed[k, half, high_rows, :] = mix_in[1, k, half]

        def later_edges(chunk):
            for more in range(CHUNK):
                mix(p_low, low_rows, CHUNK * chunk + more)
                mix(p_high, high_rows, CHUNK * chunk + more)

        def arriving_edges(chunk):
            pl.when(has_left)(lambda: to_right(chunk).wait_recv())
            pl.when(has_right)(lambda: to_left(chunk).wait_recv())
            later_edges(chunk)

        def apply(turn, edges):
            def step(chunk, so_far):
                edges(chunk)
                for more in range(CHUNK):
                    k = CHUNK * chunk + more
                    total = stencil(lambda h, rows_at: mixed[k, h, rows_at, :], back_starts, reach, back)
                    for half in range(halves):
                        resid[turn, k, half, pl.ds(RADIUS, reach), :] = total[half] * keep
                for more in range(CHUNK):
                    k = CHUNK * chunk + more
                    total = stencil(
                        lambda h, rows_at: resid[turn, k, h, rows_at, :], forth_starts, width, forth
                    )
                    so_far = tuple(
                        so_far[level * halves + half]
                        + p[level, k, :, half * LANES : (half + 1) * LANES].astype(F32) * total[half]
                        for level in range(levels)
                        for half in range(halves)
                    )
                return so_far

            summed = lax.fori_loop(
                0, chunks, step, tuple(jnp.zeros((width, LANES), F32) for _ in range(planes))
            )
            for plane in range(planes):
                part[turn, plane] = summed[plane]

        def wait_bytes(ref, sem):
            pltpu.make_async_copy(ref, ref, sem).wait()

        def start_sums(turn):
            for step in range(1, groups):
                peer = lax.rem(me + step, groups)
                remote(
                    part.at[turn, peer], gathered.at[turn, step - 1],
                    rs_send.at[turn], rs_recv.at[turn], (peer, col),
                ).start()

        def finish_sums(turn):
            wait_bytes(gathered.at[turn], rs_recv.at[turn])
            total = part[turn, me]
            for s in range(groups - 1):
                total = total + gathered[turn, s]
            full[turn, me, own, :] = total
            return total

        def start_edges(turn):
            @pl.when(has_right)
            def _():
                for step in range(groups):
                    remote(
                        full.at[turn, me, last_own, :], full.at[turn, me, low_rows, :],
                        low_send.at[turn], low_recv.at[turn], (lax.rem(me + step, groups), right),
                    ).start()

            @pl.when(has_left)
            def _():
                for step in range(groups):
                    remote(
                        full.at[turn, me, first_own, :], full.at[turn, me, high_rows, :],
                        high_send.at[turn], high_recv.at[turn], (lax.rem(me + step, groups), left),
                    ).start()

        def start_group(turn):
            spot = full.at[turn, me, own, :]
            for step in range(1, groups):
                remote(
                    spot, spot, ag_send.at[turn], ag_recv.at[turn], (lax.rem(me + step, groups), col)
                ).start()

        def others(turn):
            return full.at[turn, pl.ds(0, groups - 1), own, :]

        def finish_own(turn):
            wait_bytes(others(turn), ag_recv.at[turn])

        def finish_edges(turn):
            @pl.when(has_left)
            def _():
                wait_bytes(full.at[turn, :, low_rows, :], low_recv.at[turn])

            @pl.when(has_right)
            def _():
                wait_bytes(full.at[turn, :, high_rows, :], high_recv.at[turn])

        def send_note(which, values):
            row = jnp.zeros((1, LANES), F32)
            for at, value in enumerate(values):
                row = jnp.where(lanes8 == at, value, row)
            note[which] = row
            group_note[which, me] = row
            for step in range(1, groups):
                remote(
                    note.at[which], group_note.at[which, me],
                    note_send.at[which], note_recv.at[which], (lax.rem(me + step, groups), col),
                ).start()

        def pass_note(which):
            wait_bytes(group_note.at[which, pl.ds(0, groups - 1)], note_recv.at[which])
            total = group_note[which, 0]
            for other in range(1, groups):
                total = total + group_note[which, other]
            sums[which] = total
            block_note[which, col] = total
            for step in range(1, blocks):
                remote(
                    sums.at[which], block_note.at[which, col],
                    sum_send.at[which], sum_recv.at[which], (me, lax.rem(col + step, blocks)),
                ).start()

        def read_note(which, count):
            wait_bytes(block_note.at[which, pl.ds(0, blocks - 1)], sum_recv.at[which])
            total = block_note[which, 0]
            for other in range(1, blocks):
                total = total + block_note[which, other]
            return [
                jnp.sum(jnp.where(lanes8 == at, total, 0.0), axis=1, keepdims=True)
                for at in range(count)
            ]

        def all_of(value):
            return jnp.sum(jnp.sum(value, axis=0, keepdims=True), axis=1, keepdims=True)

        load.wait()
        for plane in range(planes):
            z[plane, own, :] = fields[0, plane, own, :]
        mix_own(True)
        beside = lax.div(col + blocks - 1, blocks) + lax.div(2 * blocks - 2 - col, blocks)
        pl.semaphore_wait(barrier, groups - 1 + beside)

        @pl.when(has_right)
        def _():
            for chunk in range(chunks):
                mixed_right(chunk).start()
            fields_right.start()

        @pl.when(has_left)
        def _():
            for chunk in range(chunks):
                mixed_left(chunk).start()
            fields_left.start()

        for copy in edge_loads:
            copy.wait()
        send_halo(0)
        say_hello(0)

        @pl.when(col == 0)
        def _():
            p_low[...] = jnp.zeros(p_low.shape, p_low.dtype)
            mix_in[0] = jnp.zeros((members, halves, HALO, LANES), F32)
            fields[:, :, low_rows, :] = jnp.zeros((2, planes, HALO, LANES), F32)
            full[:, :, low_rows, :] = jnp.zeros((3, planes, HALO, LANES), F32)

        @pl.when(col == blocks - 1)
        def _():
            p_high[...] = jnp.zeros(p_high.shape, p_high.dtype)
            mix_in[1] = jnp.zeros((members, halves, HALO, LANES), F32)
            fields[:, :, high_rows, :] = jnp.zeros((2, planes, HALO, LANES), F32)
            full[:, :, high_rows, :] = jnp.zeros((3, planes, HALO, LANES), F32)

        hear_hello(0)
        say_hello(1)

        hear_hello(1)
        say_hello(2)
        apply(0, first_edges)
        hear_hello(2)
        say_hello(3)
        start_sums(0)
        send_halo(1)

        def square(k, total):
            for half in range(halves):
                value = resid[0, k, half, own, :]
                total = total + value * value
            return total

        norm = all_of(lax.fori_loop(0, members, square, jnp.zeros((width, LANES), F32)))
        mine = finish_sums(0)
        hear_hello(3)
        say_hello(4)
        start_edges(0)
        start_group(0)
        send_halo(2, 3)
        send_note(0, [norm, all_of(fields[1, me, own, :] * mine * mine)])
        finish_own(0)

        def image_of_first(at):
            for plane in range(planes):
                z[plane, at, :] = (
                    fields[0, plane, at, :] + fields[1, plane, at, :] * full[0, plane, at, :]
                )


        image_of_first(own)
        mix_own()
        hear_hello(4)
        pass_note(0)
        finish_edges(0)

        @pl.when(has_left)
        def _():
            fields_right.wait_recv()

        @pl.when(has_right)
        def _():
            fields_left.wait_recv()

        image_of_first(low_rows)
        image_of_first(high_rows)
        apply(1, arriving_edges)
        start_sums(1)
        finish_sums(1)
        start_edges(1)
        start_group(1)
        norm_0, bend_0 = read_note(0, 2)
        curve_0 = norm_0 + bend_0
        step_0 = norm_0 / curve_0
        finish_own(1)

        def image_of_second(at):
            for plane in range(planes):
                z[plane, at, :] = (fields[0, plane, at, :] - step_0 * z[plane, at, :]) + fields[
                    1, plane, at, :
                ] * (full[0, plane, at, :] - step_0 * full[1, plane, at, :])

        image_of_second(own)
        mix_own()
        finish_edges(1)
        image_of_second(low_rows)
        image_of_second(high_rows)
        apply(2, later_edges)
        start_sums(2)

        def products(k, so_far):
            ab, ac, bb, bc, cc = so_far
            for half in range(halves):
                a = resid[0, k, half, own, :]
                b = a - step_0 * resid[1, k, half, own, :]
                c = resid[2, k, half, own, :]
                second[k, half] = b
                ab, ac, bb, bc, cc = ab + a * b, ac + a * c, bb + b * b, bc + b * c, cc + c * c
            return ab, ac, bb, bc, cc

        inner = [
            all_of(v)
            for v in lax.fori_loop(
                0, members, products, tuple(jnp.zeros((width, LANES), F32) for _ in range(5))
            )
        ]
        mine_c = finish_sums(2)
        mine_a = full[0, me, own, :]
        mine_b = mine_a - step_0 * full[1, me, own, :]
        weight = fields[1, me, own, :]
        wb, wc = weight * mine_b, weight * mine_c
        bends = [all_of(v) for v in (wb * mine_a, wc * mine_a, wb * mine_b, wc * mine_b, wc * mine_c)]
        send_note(1, inner + bends)
        start_group(2)
        pass_note(1)
        g_ab, g_ac, g_bb, g_bc, g_cc, e_ab, e_ac, e_bb, e_bc, e_cc = read_note(1, 10)
        finish_own(2)

        def form(aa, ab, ac, bb, bc, cc, u):
            a, b, c = u
            return (
                a * a * aa + b * b * bb + c * c * cc + 2.0 * (a * b * ab + a * c * ac + b * c * bc)
            )

        h = (curve_0, g_ab + e_ab, g_ac + e_ac, g_bb + e_bb, g_bc + e_bc, g_cc + e_cc)
        one = jnp.ones_like(norm_0)
        ratio_0 = g_bb / norm_0
        d1 = (ratio_0, one, 0.0 * one)
        step_1 = g_bb / form(*h, d1)
        mixing = step_1 * ratio_0 / step_0
        r2 = (-mixing, one + mixing, -step_1)
        norm_2 = form(norm_0, g_ab, g_ac, g_bb, g_bc, g_cc, r2)
        ratio_1 = norm_2 / g_bb
        d2 = tuple(r + ratio_1 * d for r, d in zip(r2, d1))
        step_2 = norm_2 / form(*h, d2)
        in_a = step_0 + step_1 * d1[0] + step_2 * d2[0]
        in_b = step_1 * d1[1] + step_2 * d2[1]
        in_c = step_1 * d1[2] + step_2 * d2[2]

        def write(step, carry):
            for more in range(UNROLL):
                k = UNROLL * step + more
                for half in range(halves):
                    control[k, :, half * LANES : (half + 1) * LANES] = (
                        in_a * resid[0, k, half, own, :]
                        + in_b * second[k, half]
                        + in_c * resid[2, k, half, own, :]
                    )
            return carry

        lax.fori_loop(0, members // UNROLL, write, 0)
        for level in range(levels):
            for half in range(halves):
                plane = level * halves + half
                a = full[0, plane, own, :]
                b = a - step_0 * full[1, plane, own, :]
                increment[level, :, half * LANES : (half + 1) * LANES] = (
                    in_a * a + in_b * b + in_c * full[2, plane, own, :]
                )

        @pl.when(has_right)
        def _():
            fields_right.wait_send()
            for chunk in range(chunks):
                to_right(chunk).wait_send()
                mixed_right(chunk).wait_send()

        @pl.when(has_left)
        def _():
            fields_left.wait_send()
            for chunk in range(chunks):
                to_left(chunk).wait_send()
                mixed_left(chunk).wait_send()

        for turn in range(3):
            wait_bytes(gathered.at[turn], rs_send.at[turn])
            wait_bytes(others(turn), ag_send.at[turn])
        for turn in range(2):

            @pl.when(has_right)
            def _():
                wait_bytes(full.at[turn, :, low_rows, :], low_send.at[turn])

            @pl.when(has_left)
            def _():
                wait_bytes(full.at[turn, :, high_rows, :], high_send.at[turn])

            wait_bytes(group_note.at[turn, pl.ds(0, groups - 1)], note_send.at[turn])
            wait_bytes(block_note.at[turn, pl.ds(0, blocks - 1)], sum_send.at[turn])

    bf16 = jnp.bfloat16
    dma = pltpu.SemaphoreType.DMA
    scratch = [
        pltpu.SMEM((TAPS,), F32),
        pltpu.SMEM((2, TAPS), jnp.int32),
        pltpu.VMEM((obs_rows, LANES), jnp.int32),
        pltpu.VMEM((obs_rows, LANES), jnp.int32),
        pltpu.VMEM((obs_rows, LANES), jnp.int32),
        pltpu.VMEM((obs_rows, LANES), F32),
        pltpu.VMEM((obs_rows, LANES), F32),
        pltpu.VMEM((levels, members, width, depth), bf16),
        pltpu.VMEM((levels, members, HALO, depth), bf16),
        pltpu.VMEM((levels, members, HALO, depth), bf16),
        pltpu.VMEM((levels, members, HALO, depth), bf16),
        pltpu.VMEM((levels, members, HALO, depth), bf16),
        pltpu.VMEM((2, members, halves, HALO, LANES), F32),
        pltpu.VMEM((2, members, halves, HALO, LANES), F32),
        pltpu.VMEM((2, planes, rows, LANES), F32),
        pltpu.VMEM((planes, rows, LANES), F32),
        pltpu.VMEM((members, halves, rows, LANES), F32),
        pltpu.VMEM((3, members, halves, rows, LANES), F32),
        pltpu.VMEM((members, halves, width, LANES), F32),
        pltpu.VMEM((3, planes, width, LANES), F32),
        pltpu.VMEM((3, groups - 1, width, LANES), F32),
        pltpu.VMEM((3, planes, rows, LANES), F32),
        pltpu.VMEM((2, 1, LANES), F32),
        pltpu.VMEM((2, groups, 1, LANES), F32),
        pltpu.VMEM((2, 1, LANES), F32),
        pltpu.VMEM((2, blocks, 1, LANES), F32),
        pltpu.SemaphoreType.REGULAR((5, 2)),
        dma((10,)),
        dma((2, chunks)), dma((2, chunks)), dma((2, chunks)), dma((2, chunks)), dma((2,)), dma((2,)),
        dma((3,)), dma((3,)), dma((3,)), dma((3,)),
        dma((2,)), dma((2,)), dma((2,)), dma((2,)),
        dma((2,)), dma((2,)), dma((2,)), dma((2,)),
    ]
    return kernel, scratch


def solution(mesh):
    groups, blocks = mesh.shape["mem"], mesh.shape["col"]

    def per_device(perturbations, loc_weights, offsets, obs_x, obs_y, obs_t, innovations, obs_rinv):
        levels, members, width, depth = perturbations.shape
        obs_rows = obs_x.shape[0] // LANES
        kernel, scratch = make_kernel(groups, blocks, levels, members, width, depth, obs_rows)
        vmem = pl.BlockSpec(memory_space=pltpu.VMEM)
        hbm = pl.BlockSpec(memory_space=pl.ANY)
        kept = pl.pallas_call(
            kernel,
            out_shape=(
                pltpu.VMEM((members, width, depth), F32),
                pltpu.VMEM((levels, width, depth), F32),
            ),
            in_specs=[hbm] * 8,
            out_specs=(vmem,) * 2,
            scratch_shapes=scratch,
            compiler_params=pltpu.CompilerParams(collective_id=0, has_side_effects=True),
        )(
            perturbations, loc_weights, offsets.T,
            *(v.reshape(obs_rows, LANES) for v in (obs_x, obs_y, obs_t, innovations, obs_rinv)),
        )

        def put_out(control, increment, control_out, increment_out, sem):
            copies = [
                pltpu.make_async_copy(control, control_out, sem.at[0]),
                pltpu.make_async_copy(increment, increment_out, sem.at[1]),
            ]
            for copy in copies:
                copy.start()
            for copy in copies:
                copy.wait()

        return pl.pallas_call(
            put_out,
            out_shape=(
                jax.ShapeDtypeStruct((members, width, depth), F32),
                jax.ShapeDtypeStruct((levels, width, depth), F32),
            ),
            in_specs=[vmem] * 2,
            out_specs=(pl.BlockSpec(memory_space=pltpu.HBM),) * 2,
            scratch_shapes=[pltpu.SemaphoreType.DMA((2,))],
        )(*(pltpu.with_memory_space_constraint(v, pltpu.VMEM) for v in kept))

    return jax.shard_map(
        per_device,
        mesh=mesh,
        in_specs=(P(None, "mem", "col", None), P(), P()) + (P("col"),) * 5,
        out_specs=(P("mem", "col", None), P(None, "col", None)),
        check_vma=False,
    )
```
